32 devices in a mesh: fsdp: 16 (over z, y, x), dp: 2 (over core).
Axes of the slice: x: 2, y: 2, z: 4, core: 2. Of those that a mesh axis runs over, the one named last changes fastest.
Arguments:
- gradients: bfloat16 [2, 64, 256, 256], P('dp', 'fsdp'), may hold values from -6 to 6
- first_moment: float32 [96, 256, 256], P('fsdp'), may hold values from -4 to 4
- second_moment: float32 [96, 256, 256], P('fsdp'), may hold values from 0.05 to 2
- left_basis: float32 [96, 256, 256], P('fsdp'), may hold values from -1 to 1, as said below
- right_basis: float32 [96, 256, 256], P('fsdp'), may hold values from -1 to 1, as said below
- shard_starts: int32 [16], replicated, may hold values from 0 to 48, as said below
- block_owners: int32 [48], replicated, may hold values from 0 to 15, as said below
Outputs:
- direction: float32 [64, 256, 256], P('fsdp')
- first_new: float32 [96, 256, 256], P('fsdp')
- second_new: float32 [96, 256, 256], P('fsdp')
The draws below stay inside these ranges and needn't reach their ends.
Inputs may be any that keep to these rules, and one draw needn't show every extreme that they name: Starts never fall and shard_starts[0] = 0; a device holds at most 4 blocks, some device exactly 4 and some none. `block_owners`: never falls; a device owns at most 6 blocks, some device exactly 6 and some none; a block's owner differs from its holder by at most 2 fsdp indices, by exactly 2 for some block in each direction. `left_basis`: each matrix is orthogonal up to float32 rounding. `right_basis`: each matrix is orthogonal up to float32 rounding.
All inputs are finite; a program needn't handle non-finite values.
Results may differ from the reference program's by a relative error of at most 0.0014.
Values may be sent and summed in bfloat16 or wider, within the bound.
No kernel may reach another device: no remote copies, remote signals or barrier semaphores. Data moves between devices by JAX's collectives and lax.ppermute only.
A program may use at most 64 MiB of HBM per device.

```python
import math
import jax
import jax.numpy as jnp
import numpy as np
from jax import lax

BS = 256
SLOTS = 4
OWN = 6
STEP = 10
NBLK = 48
N_FSDP = 16
N_DP = 2


holder_table = np.array([[4, 4, 2, 2], [4, 3, 3, 2], [4, 4, 3, 1], [4, 4, 4, 0], [4, 3, 4, 1], [4, 2, 2, 4]], dtype=np.int32)


owner_table = np.array([[6, 2, 2, 2], [6, 3, 2, 1], [6, 4, 1, 1], [6, 6, 0, 0], [6, 3, 3, 0], [6, 4, 2, 0], [6, 5, 1, 0], [6, 1, 2, 3]], dtype=np.int32)


edge_holder_table = np.array([[4, 2], [3, 3], [2, 4]], dtype=np.int32)


edge_owner_table = np.array([[3, 3], [4, 2], [2, 4], [6, 0], [0, 6]], dtype=np.int32)


def group_counts(key):
    inner = N_FSDP // 4 - 1
    middle = N_FSDP // 8 - 1
    base = jax.random.fold_in(key, 7)
    parts = jax.random.split(base, 8)
    hold_pick = jax.random.randint(parts[0], (inner,), 0, holder_table.shape[0])
    own_pick = jax.random.randint(parts[1], (inner,), 0, owner_table.shape[0])
    hold_rows = jnp.asarray(holder_table)[hold_pick]
    own_rows = jnp.asarray(owner_table)[own_pick]
    hold_keys = jax.random.split(parts[2], inner)
    own_keys = jax.random.split(parts[3], inner)
    hold_rows = jax.vmap(lambda kk, row: jax.random.permutation(kk, row))(hold_keys, hold_rows)
    own_rows = jax.vmap(lambda kk, row: jax.random.permutation(kk, row))(own_keys, own_rows)
    first_rank = jax.random.randint(parts[4], (), 0, inner - 1)
    first_group = first_rank + (first_rank >= middle).astype(jnp.int32)
    second_rank = (first_rank + 1 + jax.random.randint(parts[5], (), 0, inner - 2)) % (inner - 1)
    second_group = second_rank + (second_rank >= middle).astype(jnp.int32)
    group_ids = jnp.arange(inner)[:, None]
    hold_rows = jnp.where(group_ids == first_group, jnp.array([[4, 4, 4, 0]], jnp.int32), hold_rows)
    own_rows = jnp.where(group_ids == first_group, jnp.array([[0, 0, 6, 6]], jnp.int32), own_rows)
    hold_rows = jnp.where(group_ids == second_group, jnp.array([[0, 4, 4, 4]], jnp.int32), hold_rows)
    own_rows = jnp.where(group_ids == second_group, jnp.array([[6, 6, 0, 0]], jnp.int32), own_rows)
    hold_rows = jnp.where(group_ids == middle, jnp.array([[4, 4, 4, 0]], jnp.int32), hold_rows)
    own_rows = jnp.where(group_ids == middle, jnp.array([[0, 2, 6, 4]], jnp.int32), own_rows)
    edge_keys = jax.random.split(parts[6], 2)
    owner_keys = jax.random.split(parts[7], 2)
    edge_hold = [jnp.asarray(edge_holder_table)[jax.random.randint(edge_keys[side], (), 0, edge_holder_table.shape[0])] for side in range(2)]
    edge_own = [jnp.asarray(edge_owner_table)[jax.random.randint(owner_keys[side], (), 0, edge_owner_table.shape[0])] for side in range(2)]
    hold_counts = jnp.concatenate([edge_hold[0], hold_rows.reshape(-1), edge_hold[1]]).astype(jnp.int32)
    own_counts = jnp.concatenate([edge_own[0], own_rows.reshape(-1), edge_own[1]]).astype(jnp.int32)
    return (hold_counts, own_counts)


def draw_shard_starts(key, part):
    hold_counts, own_counts = group_counts(key)
    return (jnp.cumsum(hold_counts) - hold_counts).astype(jnp.int32)


def draw_block_owners(key, part):
    hold_counts, own_counts = group_counts(key)
    return jnp.repeat(jnp.arange(N_FSDP, dtype=jnp.int32), own_counts, total_repeat_length=NBLK).astype(jnp.int32)


def orthogonal(key, spread):
    random_part = jax.random.normal(key, (N_FSDP * OWN, BS, BS), jnp.float32) * (spread / BS ** 0.5)
    skew_part = random_part - jnp.swapaxes(random_part, 1, 2)
    identity = jnp.broadcast_to(jnp.eye(BS, dtype=jnp.float32), skew_part.shape)
    return jnp.linalg.solve(identity - skew_part, identity + skew_part)


def draw_left_basis(key, part):
    return orthogonal(jax.random.fold_in(key, 11), 0.8)


def draw_right_basis(key, part):
    return orthogonal(jax.random.fold_in(key, 13), 0.8)


def shard_levels(key, shape, cuts, smallest, high):
    def one(axis_at, blocks):
        heights = jax.random.uniform(jax.random.fold_in(jax.random.fold_in(key, 6), axis_at), (blocks,), jnp.float32, smallest / len(cuts), high / len(cuts))
        return jnp.repeat(jnp.exp(heights), shape[axis_at] // blocks).reshape((-1,) + (1,) * (len(shape) - axis_at - 1))

    level = one(*cuts[0])
    for cut in cuts[1:]:
        level = level * one(*cut)
    return level


def gaussian(own_key, dims, scale, reach, shards=(), kind=jnp.bfloat16):
    gain = shard_levels(own_key, dims, shards, -0.22, 0.18) if shards else 1.0
    result = jax.random.normal(own_key, dims, jnp.float32) * scale * gain
    return jnp.minimum(jnp.maximum(result, -reach), reach).astype(kind)


def setup_inputs(seed: int = 0) -> dict:
    streams_of = jax.random.split(jax.random.key(seed), 8)
    return {
        "gradients": gaussian(streams_of[0], (N_DP, N_FSDP * SLOTS, BS, BS), 1.0, 6.0, ((0, 2), (1, 16))),
        "first_moment": gaussian(streams_of[1], (N_FSDP * OWN, BS, BS), 0.5, 4.0, ((0, 16),), jnp.float32),
        "second_moment": jnp.clip(jnp.exp(math.log(2.0) - 3.6888794 * jax.random.uniform(streams_of[2], (N_FSDP * OWN, BS, BS), jnp.float32) ** shard_levels(streams_of[2], (N_FSDP * OWN, BS, BS), ((0, 16),), -0.2, 0.2)), 0.05, 2.0),
        "left_basis": draw_left_basis(jax.random.fold_in(streams_of[7], 71), 0),
        "right_basis": draw_right_basis(jax.random.fold_in(streams_of[7], 71), 0),
        "shard_starts": draw_shard_starts(jax.random.fold_in(streams_of[7], 71), 0),
        "block_owners": draw_block_owners(jax.random.fold_in(streams_of[7], 71), 0),
    }


beta_one = 0.9
beta_two = 0.95
epsilon = 1e-08

def soap_blocks(gradient, moment_one, moment_two, left_basis, right_basis):
    highest = lax.Precision.HIGHEST
    moment_new = beta_one * moment_one + (1.0 - beta_one) * gradient
    turned = jnp.einsum('jad,jde->jae', jnp.einsum('jba,jbd->jad', left_basis, gradient, precision=highest), right_basis, precision=highest)
    turned_moment = jnp.einsum('jad,jde->jae', jnp.einsum('jba,jbd->jad', left_basis, moment_new, precision=highest), right_basis, precision=highest)
    second_next = beta_two * moment_two + (1.0 - beta_two) * turned * turned
    bias_one = 1.0 - beta_one ** STEP
    bias_two = 1.0 - beta_two ** STEP
    scaled = turned_moment / bias_one / (jnp.sqrt(second_next / bias_two) + epsilon)
    update = jnp.einsum('jad,jed->jae', jnp.einsum('jab,jbd->jad', left_basis, scaled, precision=highest), right_basis, precision=highest)
    return (moment_new, second_next, update)

def reference(gradients, first_moment, second_moment, left_basis, right_basis, shard_starts, block_owners):
    block_ids = jnp.arange(NBLK, dtype=jnp.int32)
    holder = (jnp.searchsorted(shard_starts, block_ids, side='right') - 1).astype(jnp.int32)
    hold_row = (holder * SLOTS + block_ids - shard_starts[holder]).astype(jnp.int32)
    first_owned = jnp.searchsorted(block_owners, block_owners, side='left').astype(jnp.int32)
    own_row = (block_owners * OWN + block_ids - first_owned).astype(jnp.int32)
    summed = lax.optimization_barrier(jnp.sum(gradients.astype(jnp.float32), axis=0)).astype(jnp.bfloat16)
    gradient = summed[hold_row].astype(jnp.float32)
    moment_new, second_next, update = soap_blocks(gradient, first_moment[own_row], second_moment[own_row], left_basis[own_row], right_basis[own_row])
    blank_hold = jnp.zeros((N_FSDP * SLOTS, BS, BS), jnp.float32)
    blank_own = jnp.zeros((N_FSDP * OWN, BS, BS), jnp.float32)
    direction = blank_hold.at[hold_row].set(update)
    first_new = blank_own.at[own_row].set(moment_new)
    second_new = blank_own.at[own_row].set(second_next)
    return (direction, first_new, second_new)
```

```python
import functools

import jax
import jax.numpy as jnp
from jax import lax
from jax.experimental import pallas as pl
from jax.experimental.pallas import tpu as pltpu
from jax.sharding import PartitionSpec as P

STEP = 10
CODE_ROWS = 16
CODE_STEPS = 128.0

beta_one = 0.9
beta_two = 0.95
epsilon = 1e-08

HERE, SIDE, CROSS, FLIP, FAR = range(5)


def exchange(value, pairs):
    return lax.ppermute(value, "fsdp", pairs + [(b, a) for a, b in pairs])


def partner_pairs(devices):
    side = [(i, i + 1) for i in range(0, devices - 1, 2)]
    cross = [(i, i + 1) for i in range(1, devices - 1, 2)]
    flip = [(i, i + 2) for i in range(devices - 2) if not i & 2]
    far = [(i, i + 2) for i in range(devices - 2) if i & 2]
    return (side, cross, flip, far)


def swap_cores(value):
    return lax.ppermute(value, "dp", [(0, 1), (1, 0)])


def partner_kind(me, other):
    step = other - me
    near = jnp.where(other == me ^ 1, SIDE, CROSS)
    distant = jnp.where(other == me ^ 2, FLIP, FAR)
    return jnp.where(step == 0, HERE, jnp.where(jnp.abs(step) == 1, near, distant))


def tables(shard_starts, block_owners, me, slot_count, owned_slots):
    devices = shard_starts.shape[0]
    total = block_owners.shape[0]
    ids = jnp.arange(devices, dtype=jnp.int32)
    first = jnp.sum((block_owners < me).astype(jnp.int32))
    count = jnp.sum((block_owners == me).astype(jnp.int32))
    owned = first + jnp.arange(owned_slots, dtype=jnp.int32)
    begun = shard_starts[None, :] <= owned[:, None]
    holder = jnp.sum(begun.astype(jnp.int32), axis=1) - 1
    slot = owned - jnp.max(jnp.where(begun, shard_starts[None, :], 0), axis=1)
    owned_kind = jnp.where(jnp.arange(owned_slots) < count, partner_kind(me, holder), -1)
    start = jnp.sum(jnp.where(ids == me, shard_starts, 0))
    end = jnp.sum(jnp.where(ids == me + 1, shard_starts, 0)) + jnp.where(me == devices - 1, total, 0)
    held = start + jnp.arange(slot_count, dtype=jnp.int32)
    blocks = jnp.arange(total, dtype=jnp.int32)
    owner = jnp.sum(jnp.where(blocks[None, :] == held[:, None], block_owners[None, :], 0), axis=1)
    held_kind = jnp.where(held < end, partner_kind(me, owner), -1)
    return (
        owned_kind.astype(jnp.int32),
        jnp.clip(slot, 0, slot_count - 1).astype(jnp.int32),
        held_kind.astype(jnp.int32),
    )


def split(value):
    high = value.astype(jnp.bfloat16)
    return high, (value - high.astype(jnp.float32)).astype(jnp.bfloat16)


def product(a, b, dims):
    return lax.dot_general(a, b, (dims, ((), ())), preferred_element_type=jnp.float32)


def product3(a, b, dims):
    return product(a[0], b[0], dims) + (product(a[0], b[1], dims) + product(a[1], b[0], dims))


TN = ((0,), (0,))
NN = ((1,), (0,))
NT = ((1,), (1,))


def moment_kernel(moment_ref, left_ref, right_ref, out_ref):
    left, right = split(left_ref[0]), split(right_ref[0])
    half = product3(left, split(moment_ref[0]), TN)
    out_ref[0] = product3(split(half), right, NN)


def turn_moment(first_moment, left_basis, right_basis):
    count, width, _ = first_moment.shape
    spec = pl.BlockSpec((1, width, width), lambda j: (j, 0, 0))
    return pl.pallas_call(
        moment_kernel,
        grid=(count,),
        in_specs=[spec] * 3,
        out_specs=spec,
        out_shape=jax.ShapeDtypeStruct(first_moment.shape, jnp.float32),
        cost_estimate=pl.CostEstimate(
            flops=12 * count * width**3, bytes_accessed=16 * count * width**2, transcendentals=0
        ),
        name="turn_moment",
    )(first_moment, left_basis, right_basis)


def collect_kernel(kind_ref, slot_ref, *refs, rows, extra):
    sources, out_ref, sem = refs[:5], refs[5], refs[6]
    count = kind_ref.shape[0]

    def each(j, act):
        for kind in range(5):

            @pl.when(kind_ref[j] == kind)
            def _():
                act(
                    pltpu.make_async_copy(
                        sources[kind].at[pl.ds(pl.multiple_of(slot_ref[j] * rows, rows), rows)],
                        out_ref.at[pl.ds(j * rows, rows)],
                        sem.at[j],
                    )
                )

    for j in range(count):
        each(j, lambda copy: copy.start())
    for j in range(count):
        each(j, lambda copy: copy.wait())


def collect(kind, slot, sources):
    count = kind.shape[0]
    rows, width = sources[0].shape[1:]
    flat = [source.reshape(-1, width) for source in sources]
    out = pl.pallas_call(
        functools.partial(collect_kernel, rows=rows, extra=0),
        in_specs=[pl.BlockSpec(memory_space=pltpu.SMEM)] * 2 + [pl.BlockSpec(memory_space=pl.ANY)] * 5,
        out_specs=pl.BlockSpec(memory_space=pltpu.VMEM),
        out_shape=jax.ShapeDtypeStruct((count * rows, width), sources[0].dtype),
        scratch_shapes=[pltpu.SemaphoreType.DMA((count,))],
        name="collect",
    )(kind, slot, *flat)
    return out.reshape(count, rows, width)


def step_kernel(
    kind_ref,
    slot_ref,
    place_ref,
    mine_ref,
    other_ref,
    moment_ref,
    second_ref,
    left_ref,
    right_ref,
    turned_ref,
    first_out,
    second_out,
    *refs,
):
    sends, codes = refs[:5], refs[5]
    j = pl.program_id(0)
    live = kind_ref[j] >= 0
    half = mine_ref.shape[1]
    here = pl.multiple_of(place_ref[0] * half, half)
    there = pl.multiple_of((1 - place_ref[0]) * half, half)
    parts = ((here, mine_ref), (there, other_ref))

    @pl.when(j == 0)
    def _():
        codes[...] = jnp.zeros_like(codes)

    @pl.when(jnp.logical_not(live))
    def _():
        first_out[...] = jnp.zeros_like(first_out)
        second_out[...] = jnp.zeros_like(second_out)

    @pl.when(live)
    def _():
        right = split(right_ref[0])
        half_turned = None
        for at, part in parts:
            gradient = part[0]
            first_out[0, pl.ds(at, half)] = beta_one * moment_ref[0, pl.ds(at, half)] + (
                1.0 - beta_one
            ) * gradient.astype(jnp.float32)
            high, low = split(left_ref[0, pl.ds(at, half)])
            term = product(high, gradient, TN) + product(low, gradient, TN)
            half_turned = term if half_turned is None else half_turned + term
        turned = product3(split(half_turned), right, NN)
        second = beta_two * second_ref[0] + (1.0 - beta_two) * turned * turned
        second_out[0] = second
        turned_moment = beta_one * turned_ref[0] + (1.0 - beta_one) * turned
        bias_one = 1.0 - beta_one**STEP
        bias_two = 1.0 - beta_two**STEP
        scaled = turned_moment / bias_one / (jnp.sqrt(second / bias_two) + epsilon)
        back = product3(split(left_ref[0, pl.ds(here, half)]), split(scaled), NN)
        update = product3(split(back), right, NT)
        peak = jnp.max(jnp.abs(update), axis=0, keepdims=True)
        code = jnp.ceil(jnp.log2(jnp.maximum(peak, 1e-30) * (1.0 / 32000.0)) * CODE_STEPS)
        coded = jnp.round(update * jnp.exp2(code * (-1.0 / CODE_STEPS)))
        coded = jnp.clip(coded, -32767.0, 32767.0).astype(jnp.int32).astype(jnp.int16)
        slot = slot_ref[j]
        rows = pl.ds(pl.multiple_of(slot * half, half), half)
        spots = lax.broadcasted_iota(jnp.int32, codes.shape[1:], 0)
        for kind in range(5):

            @pl.when(kind_ref[j] == kind)
            def _():
                sends[kind][rows] = coded
                codes[kind] = jnp.where(spots == slot, code.astype(jnp.int32), codes[kind])

    @pl.when(j == pl.num_programs(0) - 1)
    def _():
        for kind in range(5):
            top = sends[kind].shape[0] - CODE_ROWS
            sends[kind][pl.ds(top, CODE_ROWS)] = codes[kind].astype(jnp.int16)


def soap_step(kind, slot, place, mine, other, moment, second, left, right, turned, slot_count):
    count, width, _ = moment.shape
    half = mine.shape[1]
    full = pl.BlockSpec((1, width, width), lambda j, *_: (j, 0, 0))
    part = pl.BlockSpec((1, half, width), lambda j, *_: (j, 0, 0))
    send_rows = slot_count * half + CODE_ROWS
    send = pl.BlockSpec((send_rows, width), lambda j, *_: (0, 0))
    return pl.pallas_call(
        step_kernel,
        grid_spec=pltpu.PrefetchScalarGridSpec(
            num_scalar_prefetch=3,
            grid=(count,),
            in_specs=[part, part, full, full, full, full, full],
            out_specs=[full, full] + [send] * 5,
            scratch_shapes=[pltpu.VMEM((5, CODE_ROWS, width), jnp.int32)],
        ),
        out_shape=[jax.ShapeDtypeStruct(moment.shape, jnp.float32)] * 2
        + [jax.ShapeDtypeStruct((send_rows, width), jnp.int16)] * 5,
        name="soap_step",
    )(kind, slot, place, mine, other, moment, second, left, right, turned)


def gather_kernel(kind_ref, *refs, half):
    sources, out_ref, codes, sem, code_sem = refs[:5], refs[5], refs[6], refs[7], refs[8]
    count = kind_ref.shape[0]
    top = count * half

    def code_copy(kind):
        return pltpu.make_async_copy(
            sources[kind].at[pl.ds(top, CODE_ROWS)], codes.at[kind], code_sem.at[kind]
        )

    def each(s, act):
        for kind in range(5):

            @pl.when(kind_ref[s] == kind)
            def _():
                rows = pl.ds(s * half, half)
                act(pltpu.make_async_copy(sources[kind].at[rows], out_ref.at[rows], sem.at[s]))

    for kind in range(5):
        code_copy(kind).start()
    for s in range(count):
        each(s, lambda copy: copy.start())
    for kind in range(5):
        code_copy(kind).wait()
    spots = lax.broadcasted_iota(jnp.int32, codes.shape[1:], 0)
    chosen = jnp.zeros(codes.shape[1:], jnp.int32)
    for s in range(count):
        for kind in range(5):
            use = jnp.logical_and(spots == s, kind_ref[s] == kind)
            chosen = jnp.where(use, codes[kind].astype(jnp.int32), chosen)
    out_ref[pl.ds(top, CODE_ROWS)] = chosen.astype(jnp.int16)
    for s in range(count):
        each(s, lambda copy: copy.wait())


def gather_held(kind, sources):
    count = kind.shape[0]
    rows, width = sources[0].shape
    half = (rows - CODE_ROWS) // count
    return pl.pallas_call(
        functools.partial(gather_kernel, half=half),
        in_specs=[pl.BlockSpec(memory_space=pltpu.SMEM)] + [pl.BlockSpec(memory_space=pl.ANY)] * 5,
        out_specs=pl.BlockSpec(memory_space=pltpu.VMEM),
        out_shape=jax.ShapeDtypeStruct((rows, width), sources[0].dtype),
        scratch_shapes=[
            pltpu.VMEM((5, CODE_ROWS, width), jnp.int16),
            pltpu.SemaphoreType.DMA((count,)),
            pltpu.SemaphoreType.DMA((5,)),
        ],
        name="gather_held",
    )(kind, *sources)


def decode_kernel(kind_ref, place_ref, mine_ref, other_ref, mine_code, other_code, out_ref):
    s = pl.program_id(0)
    half = mine_ref.shape[0]
    live = kind_ref[s] >= 0
    spots = lax.broadcasted_iota(jnp.int32, mine_code.shape, 0)
    for place, coded, codes in ((place_ref[0], mine_ref, mine_code), (1 - place_ref[0], other_ref, other_code)):
        picked = jnp.where(spots == s, codes[...].astype(jnp.int32).astype(jnp.float32), 0.0)
        scale = jnp.exp2(jnp.sum(picked, axis=0, keepdims=True) * (1.0 / CODE_STEPS))
        value = coded[...].astype(jnp.int32).astype(jnp.float32) * scale
        out_ref[0, pl.ds(pl.multiple_of(place * half, half), half)] = jnp.where(live, value, 0.0)


def decode(kind, place, mine, other, width):
    count = kind.shape[0]
    half = (mine.shape[0] - CODE_ROWS) // count
    body_spec = pl.BlockSpec((half, width), lambda s, *_: (s, 0))
    code_spec = pl.BlockSpec((CODE_ROWS, width), lambda s, *_: (count * half // CODE_ROWS, 0))
    return pl.pallas_call(
        decode_kernel,
        grid_spec=pltpu.PrefetchScalarGridSpec(
            num_scalar_prefetch=2,
            grid=(count,),
            in_specs=[body_spec, body_spec, code_spec, code_spec],
            out_specs=pl.BlockSpec((1, 2 * half, width), lambda s, *_: (s, 0, 0)),
        ),
        out_shape=jax.ShapeDtypeStruct((count, 2 * half, width), jnp.float32),
        name="decode",
    )(kind, place, mine, other, mine, other)


def body(
    gradients, first_moment, second_moment, left_basis, right_basis, shard_starts, block_owners
):
    me = lax.axis_index("fsdp").astype(jnp.int32)
    core = lax.axis_index("dp").astype(jnp.int32)
    devices = lax.axis_size("fsdp")
    slot_count, width = gradients.shape[1], gradients.shape[3]
    owned_slots = first_moment.shape[0]
    half = width // lax.axis_size("dp")
    side, cross, flip, far = partner_pairs(devices)
    own_kind, own_slot, held_kind = tables(shard_starts, block_owners, me, slot_count, owned_slots)
    place = core.reshape(1)

    replica = gradients[0]
    twin = swap_cores(replica)

    def rows_of(value):
        return lax.dynamic_slice_in_dim(value, core * half, half, 1).astype(jnp.float32)

    summed = (rows_of(replica) + rows_of(twin)).astype(jnp.bfloat16)
    by_side = exchange(summed, side)
    by_flip = exchange(summed, flip)
    by_cross = exchange(summed, cross)
    by_far = exchange(summed, far)
    turned = turn_moment(first_moment, left_basis, right_basis)
    mine = collect(own_kind, own_slot, (summed, by_side, by_cross, by_flip, by_far))
    other = swap_cores(mine)
    first_new, second_new, keep, to_side, to_cross, to_flip, to_far = soap_step(
        own_kind,
        own_slot,
        place,
        mine,
        other,
        first_moment,
        second_moment,
        left_basis,
        right_basis,
        turned,
        slot_count,
    )
    sent = (
        keep,
        exchange(to_side, side),
        exchange(to_cross, cross),
        exchange(to_flip, flip),
        exchange(to_far, far),
    )
    coded = gather_held(held_kind, sent)
    direction = decode(held_kind, place, coded, swap_cores(coded), width)
    return (direction, first_new, second_new)


def solution(mesh):
    in_specs = (
        P("dp", "fsdp", None, None),
        P("fsdp", None, None),
        P("fsdp", None, None),
        P("fsdp", None, None),
        P("fsdp", None, None),
        P(),
        P(),
    )
    out_specs = (P("fsdp", None, None), P("fsdp", None, None), P("fsdp", None, None))
    return jax.shard_map(body, mesh=mesh, in_specs=in_specs, out_specs=out_specs, check_vma=False)
```

```python
import jax
import jax.numpy as jnp
from jax import lax
from jax.experimental import pallas as pl
from jax.experimental.pallas import tpu as pltpu
from jax.sharding import PartitionSpec as P


STEP = 10
CODE_ROWS = 16
CODE_STEPS = 128.0
GROUP = 3
SMALL_VMEM = 12 * 2**20
STEP_VMEM = 28 * 2**20

beta_one = 0.9
beta_two = 0.95
epsilon = 1e-08

HERE, SIDE, CROSS, FLIP, FAR = range(5)


def exchange(value, pairs):
    return lax.ppermute(value, "fsdp", pairs + [(b, a) for a, b in pairs])


def partner_pairs(devices):
    side = [(i, i + 1) for i in range(0, devices - 1, 2)]
    cross = [(i, i + 1) for i in range(1, devices - 1, 2)]
    flip = [(i, i + 2) for i in range(devices - 2) if not i & 2]
    far = [(i, i + 2) for i in range(devices - 2) if i & 2]
    return (side, cross, flip, far)


def swap_cores(value):
    return lax.ppermute(value, "dp", [(0, 1), (1, 0)])


def partner_kind(me, other):
    step = other - me
    near = jnp.where(other == me ^ 1, SIDE, CROSS)
    distant = jnp.where(other == me ^ 2, FLIP, FAR)
    return jnp.where(step == 0, HERE, jnp.where(jnp.abs(step) == 1, near, distant))


def tables(shard_starts, block_owners, me, slot_count, owned_slots):
    devices = shard_starts.shape[0]
    total = block_owners.shape[0]
    ids = jnp.arange(devices, dtype=jnp.int32)
    first = jnp.sum((block_owners < me).astype(jnp.int32))
    count = jnp.sum((block_owners == me).astype(jnp.int32))
    owned = first + jnp.arange(owned_slots, dtype=jnp.int32)
    begun = shard_starts[None, :] <= owned[:, None]
    holder = jnp.sum(begun.astype(jnp.int32), axis=1) - 1
    slot = owned - jnp.max(jnp.where(begun, shard_starts[None, :], 0), axis=1)
    owned_kind = jnp.where(jnp.arange(owned_slots) < count, partner_kind(me, holder), -1)
    start = jnp.sum(jnp.where(ids == me, shard_starts, 0))
    end = jnp.sum(jnp.where(ids == me + 1, shard_starts, 0)) + jnp.where(me == devices - 1, total, 0)
    held = start + jnp.arange(slot_count, dtype=jnp.int32)
    blocks = jnp.arange(total, dtype=jnp.int32)
    owner = jnp.sum(jnp.where(blocks[None, :] == held[:, None], block_owners[None, :], 0), axis=1)
    held_kind = jnp.where(held < end, partner_kind(me, owner), -1)
    return (
        owned_kind.astype(jnp.int32),
        jnp.clip(slot, 0, slot_count - 1).astype(jnp.int32),
        held_kind.astype(jnp.int32),
    )


def split(value):
    high = value.astype(jnp.bfloat16)
    return high, (value - high.astype(jnp.float32)).astype(jnp.bfloat16)


def product(a, b, dims):
    return lax.dot_general(a, b, (dims, ((), ())), preferred_element_type=jnp.float32)


def product3(a, b, dims):
    left = jnp.concatenate((a[0], a[0], a[1]), axis=dims[0][0])
    right = jnp.concatenate((b[0], b[1], b[0]), axis=dims[1][0])
    return product(left, right, dims)


NN = ((1,), (0,))
NT = ((1,), (1,))


def moment_kernel(moment_ref, left_ref, right_ref, out_ref, *refs):
    left_high, left_low, right_high, right_low = refs
    flipped, right = split(left_ref[0].T), split(right_ref[0])
    half = product3(split(moment_ref[0]), right, NN)
    out_ref[0] = product3(flipped, split(half), NN)
    left_high[0], left_low[0] = flipped
    right_high[0], right_low[0] = right


def in_hbm(*values):
    return tuple(pltpu.with_memory_space_constraint(value, pltpu.HBM) for value in values)


def turn_moment(first_moment, left_basis, right_basis):
    count, width, _ = first_moment.shape
    spec = pl.BlockSpec((1, width, width), lambda j: (j, 0, 0))
    short = pltpu.HBM(first_moment.shape, jnp.bfloat16)
    return pl.pallas_call(
        moment_kernel,
        grid=(count,),
        in_specs=[spec] * 3,
        out_specs=[spec] * 5,
        out_shape=[pltpu.HBM(first_moment.shape, jnp.float32)] + [short] * 4,
        compiler_params=pltpu.CompilerParams(vmem_limit_bytes=SMALL_VMEM),
        cost_estimate=pl.CostEstimate(
            flops=12 * count * width**3, bytes_accessed=24 * count * width**2, transcendentals=0
        ),
        name="turn_moment",
    )(*in_hbm(first_moment, left_basis, right_basis))


def collect_kernel(kind_ref, slot_ref, *refs):
    sources, out_ref = refs[:5], refs[5]
    for j in range(out_ref.shape[0]):
        for kind in range(5):

            @pl.when(kind_ref[j] == kind)
            def _():
                out_ref[j] = sources[kind][slot_ref[j]]


def collect(kind, slot, sources):
    count = kind.shape[0]
    return pl.pallas_call(
        collect_kernel,
        in_specs=[pl.BlockSpec(memory_space=pltpu.SMEM)] * 2
        + [pl.BlockSpec(memory_space=pltpu.VMEM)] * 5,
        out_specs=pl.BlockSpec(memory_space=pltpu.VMEM),
        out_shape=jax.ShapeDtypeStruct((count,) + sources[0].shape[1:], sources[0].dtype),
        compiler_params=pltpu.CompilerParams(vmem_limit_bytes=SMALL_VMEM),
        name="collect",
    )(kind, slot, *sources)


def step_kernel(
    kind_ref,
    slot_ref,
    place_ref,
    mine_ref,
    other_ref,
    moment_ref,
    second_ref,
    rows_ref,
    turned_ref,
    left_high,
    left_low,
    right_high,
    right_low,
    first_out,
    second_out,
    *refs,
):
    sends, codes, grads = refs[:5], refs[5], refs[6]
    step = pl.program_id(0)
    group, half = mine_ref.shape[:2]
    here = pl.multiple_of(place_ref[0] * half, half)
    there = pl.multiple_of((1 - place_ref[0]) * half, half)
    every = range(group)
    live = [kind_ref[step * group + g] >= 0 for g in every]

    @pl.when(step == 0)
    def _():
        codes[...] = jnp.zeros_like(codes)

    for g in every:
        grads[g, pl.ds(here, half)] = mine_ref[g]
        grads[g, pl.ds(there, half)] = other_ref[g]
    right = [(right_high[g], right_low[g]) for g in every]
    first = [
        product(jnp.concatenate((grads[g],) * 2, axis=1), jnp.concatenate(right[g], axis=0), NN)
        for g in every
    ]
    for g in every:
        moment = beta_one * moment_ref[g] + (1.0 - beta_one) * grads[g].astype(jnp.float32)
        first_out[g] = jnp.where(live[g], moment, 0.0)
    turned = [product3((left_high[g], left_low[g]), split(first[g]), NN) for g in every]
    bias_one = 1.0 - beta_one**STEP
    bias_two = 1.0 - beta_two**STEP
    scaled = []
    for g in every:
        second = beta_two * second_ref[g] + (1.0 - beta_two) * turned[g] * turned[g]
        second_out[g] = jnp.where(live[g], second, 0.0)
        turned_moment = beta_one * turned_ref[g] + (1.0 - beta_one) * turned[g]
        scaled.append(
            split(
                turned_moment * (1.0 / bias_one) / (jnp.sqrt(second * (1.0 / bias_two)) + epsilon)
            )
        )
    back = [product3(split(rows_ref[g]), scaled[g], NN) for g in every]
    update = [product3(split(back[g]), right[g], NT) for g in every]
    spots = lax.broadcasted_iota(jnp.int32, codes.shape[1:], 0)
    for g in every:
        peak = jnp.max(jnp.abs(update[g]), axis=0, keepdims=True)
        code = jnp.ceil(jnp.log2(jnp.maximum(peak, 1e-30) * (1.0 / 32000.0)) * CODE_STEPS)
        coded = jnp.round(update[g] * jnp.exp2(code * (-1.0 / CODE_STEPS)))
        coded = jnp.clip(coded, -32767.0, 32767.0).astype(jnp.int32).astype(jnp.int16)
        slot = slot_ref[step * group + g]
        rows = pl.ds(pl.multiple_of(slot * half, half), half)
        for kind in range(5):

            @pl.when(kind_ref[step * group + g] == kind)
            def _():
                sends[kind][rows] = coded
                codes[kind] = jnp.where(spots == slot, code.astype(jnp.int32), codes[kind])

    @pl.when(step == pl.num_programs(0) - 1)
    def _():
        for kind in range(5):
            top = sends[kind].shape[0] - CODE_ROWS
            sends[kind][pl.ds(top, CODE_ROWS)] = codes[kind].astype(jnp.int16)


def soap_step(kind, slot, place, mine, other, moment, second, left, turned, slot_count):
    count, width, _ = moment.shape
    half = mine.shape[1]
    group = GROUP if count % GROUP == 0 else 1
    full = pl.BlockSpec((group, width, width), lambda j, *_: (j, 0, 0))
    part = pl.BlockSpec((group, half, width), lambda j, *_: (j, 0, 0))
    rows = pl.BlockSpec((group, half, width), lambda j, kinds, slots, place: (j, place[0], 0))
    send_rows = slot_count * half + CODE_ROWS
    send = pl.BlockSpec((send_rows, width), lambda j, *_: (0, 0))
    return pl.pallas_call(
        step_kernel,
        grid_spec=pltpu.PrefetchScalarGridSpec(
            num_scalar_prefetch=3,
            grid=(count // group,),
            in_specs=[part, part, full, full, rows] + [full] * 5,
            out_specs=[full, full] + [send] * 5,
            scratch_shapes=[
                pltpu.VMEM((5, CODE_ROWS, width), jnp.int32),
                pltpu.VMEM((group, width, width), jnp.bfloat16),
            ],
        ),
        out_shape=[jax.ShapeDtypeStruct(moment.shape, jnp.float32)] * 2
        + [jax.ShapeDtypeStruct((send_rows, width), jnp.int16)] * 5,
        compiler_params=pltpu.CompilerParams(vmem_limit_bytes=STEP_VMEM),
        name="soap_step",
    )(kind, slot, place, mine, other, *in_hbm(moment, second, left, *turned))


def gather_kernel(kind_ref, *refs):
    sources, out_ref = refs[:5], refs[5]
    count = kind_ref.shape[0]
    top = out_ref.shape[0] - CODE_ROWS
    half = top // count
    spots = lax.broadcasted_iota(jnp.int32, (CODE_ROWS, out_ref.shape[1]), 0)
    chosen = jnp.zeros(spots.shape, jnp.int32)
    for s in range(count):
        for kind in range(5):

            @pl.when(kind_ref[s] == kind)
            def _():
                rows = pl.ds(s * half, half)
                out_ref[rows] = sources[kind][rows]

    for kind in range(5):
        code = sources[kind][pl.ds(top, CODE_ROWS)].astype(jnp.int32)
        for s in range(count):
            chosen = jnp.where((spots == s) & (kind_ref[s] == kind), code, chosen)
    out_ref[pl.ds(top, CODE_ROWS)] = chosen.astype(jnp.int16)


def gather_held(kind, sources):
    return pl.pallas_call(
        gather_kernel,
        in_specs=[pl.BlockSpec(memory_space=pltpu.SMEM)]
        + [pl.BlockSpec(memory_space=pltpu.VMEM)] * 5,
        out_specs=pl.BlockSpec(memory_space=pltpu.VMEM),
        out_shape=jax.ShapeDtypeStruct(sources[0].shape, sources[0].dtype),
        compiler_params=pltpu.CompilerParams(vmem_limit_bytes=SMALL_VMEM),
        name="gather_held",
    )(kind, *sources)


def decode_kernel(kind_ref, place_ref, mine_ref, other_ref, out_ref, scales):
    s = pl.program_id(0)
    count = kind_ref.shape[0]
    top = mine_ref.shape[0] - CODE_ROWS
    half = top // count
    live = kind_ref[s] >= 0
    both = ((place_ref[0], mine_ref), (1 - place_ref[0], other_ref))

    @pl.when(s == 0)
    def _():
        for i, (_, coded) in enumerate(both):
            code = coded[pl.ds(top, CODE_ROWS)].astype(jnp.int32).astype(jnp.float32)
            scales[i] = jnp.exp2(code * (1.0 / CODE_STEPS))

    for i, (place, coded) in enumerate(both):
        rows = pl.ds(pl.multiple_of(s * half, half), half)
        value = coded[rows].astype(jnp.int32).astype(jnp.float32) * scales[i, pl.ds(s, 1)]
        to = pl.ds(pl.multiple_of(place * half, half), half)
        out_ref[0, to] = jnp.where(live, value, 0.0)


def decode(kind, place, mine, other, width):
    count = kind.shape[0]
    half = (mine.shape[0] - CODE_ROWS) // count
    whole = pl.BlockSpec(memory_space=pltpu.VMEM)
    return pl.pallas_call(
        decode_kernel,
        grid=(count,),
        in_specs=[pl.BlockSpec(memory_space=pltpu.SMEM)] * 2 + [whole, whole],
        out_specs=pl.BlockSpec((1, 2 * half, width), lambda s: (s, 0, 0)),
        out_shape=jax.ShapeDtypeStruct((count, 2 * half, width), jnp.float32),
        scratch_shapes=[pltpu.VMEM((2, CODE_ROWS, width), jnp.float32)],
        compiler_params=pltpu.CompilerParams(vmem_limit_bytes=SMALL_VMEM),
        name="decode",
    )(kind, place, mine, other)


def body(
    gradients, first_moment, second_moment, left_basis, right_basis, shard_starts, block_owners
):
    me = lax.axis_index("fsdp").astype(jnp.int32)
    core = lax.axis_index("dp").astype(jnp.int32)
    devices = lax.axis_size("fsdp")
    slot_count, width = gradients.shape[1], gradients.shape[3]
    owned_slots = first_moment.shape[0]
    half = width // lax.axis_size("dp")
    side, cross, flip, far = partner_pairs(devices)
    place = core.reshape(1)

    replica = gradients[0]
    twin = swap_cores(replica)

    def rows_of(value):
        return lax.dynamic_slice_in_dim(value, core * half, half, 1).astype(jnp.float32)

    summed = (rows_of(replica) + rows_of(twin)).astype(jnp.bfloat16)
    summed, shard_starts, block_owners = lax.optimization_barrier(
        (summed, shard_starts, block_owners)
    )
    own_kind, own_slot, held_kind = tables(shard_starts, block_owners, me, slot_count, owned_slots)
    by_flip = exchange(summed, flip)
    by_cross = exchange(summed, cross)
    by_far = exchange(summed, far)
    by_side = exchange(summed, side)
    turned = turn_moment(first_moment, left_basis, right_basis)
    mine = collect(own_kind, own_slot, (summed, by_side, by_cross, by_flip, by_far))
    other = swap_cores(mine)
    first_new, second_new, keep, to_side, to_cross, to_flip, to_far = soap_step(
        own_kind,
        own_slot,
        place,
        mine,
        other,
        first_moment,
        second_moment,
        left_basis,
        turned,
        slot_count,
    )
    sent = (
        keep,
        exchange(to_side, side),
        exchange(to_cross, cross),
        exchange(to_flip, flip),
        exchange(to_far, far),
    )
    coded = gather_held(held_kind, sent)
    direction = decode(held_kind, place, coded, swap_cores(coded), width)
    return (direction, first_new, second_new)


def solution(mesh):
    in_specs = (
        P("dp", "fsdp", None, None),
        P("fsdp", None, None),
        P("fsdp", None, None),
        P("fsdp", None, None),
        P("fsdp", None, None),
        P(),
        P(),
    )
    out_specs = (P("fsdp", None, None), P("fsdp", None, None), P("fsdp", None, None))
    return jax.shard_map(body, mesh=mesh, in_specs=in_specs, out_specs=out_specs, check_vma=False)
```

```python
import jax
import jax.numpy as jnp
from jax import lax
from jax.experimental import pallas as pl
from jax.experimental.pallas import tpu as pltpu
from jax.sharding import PartitionSpec as P


REACH = 2
STEP = 10
CODE_ROWS = 16
CODE_STEPS = 128.0
PREPARE_GROUP = 3
GROUP = 3
SMALL_VMEM = 12 * 2**20
STEP_VMEM = 28 * 2**20

beta_one = 0.9
beta_two = 0.95
epsilon = 1e-08
bias_one = 1.0 - beta_one**STEP
bias_two = 1.0 - beta_two**STEP

HERE, SIDE, CROSS, FLIP, FAR = range(5)


def exchange(value, pairs):
    return lax.ppermute(value, "fsdp", pairs + [(b, a) for a, b in pairs])


def partner_pairs(devices):
    side = [(i, i + 1) for i in range(0, devices - 1, 2)]
    cross = [(i, i + 1) for i in range(1, devices - 1, 2)]
    flip = [(i, i + 2) for i in range(devices - 2) if not i & 2]
    far = [(i, i + 2) for i in range(devices - 2) if i & 2]
    return (side, cross, flip, far)


def swap_cores(value):
    return lax.ppermute(value, "dp", [(0, 1), (1, 0)])


def partner_kind(me, other):
    step = jnp.abs(other - me)
    near = jnp.where(other == me ^ 1, SIDE, CROSS)
    distant = jnp.where(other == me ^ 2, FLIP, FAR)
    return jnp.where(step == 0, HERE, jnp.where(step == 1, near, distant))


def in_hbm(*values):
    return tuple(pltpu.with_memory_space_constraint(value, pltpu.HBM) for value in values)


def in_vmem(*values):
    return tuple(pltpu.with_memory_space_constraint(value, pltpu.VMEM) for value in values)


def tables_kernel(me_ref, starts_ref, owners_ref, owned_kind, owned_slot, held_kind):
    me = me_ref[0]
    devices, total = starts_ref.shape[0], owners_ref.shape[0]

    def tally(b, sums):
        owner = owners_ref[b]
        return sums[0] + (owner < me).astype(jnp.int32), sums[1] + (owner == me).astype(jnp.int32)

    zero = jnp.int32(0)
    first, count = lax.fori_loop(0, total, tally, (zero, zero))
    near = [me + step for step in range(-REACH, REACH + 1)]
    begins = [starts_ref[jnp.clip(device, 0, devices - 1)] for device in near]
    for j in range(owned_kind.shape[0]):
        holder, start = near[0], begins[0]
        for device, begin in zip(near, begins):
            reached = (device >= 0) & (device < devices) & (begin <= first + j)
            holder = jnp.where(reached, device, holder)
            start = jnp.where(reached, begin, start)
        owned_kind[j] = jnp.where(j < count, partner_kind(me, holder), -1)
        owned_slot[j] = jnp.clip(first + j - start, 0, held_kind.shape[0] - 1)
    start = starts_ref[me]
    end = jnp.where(me + 1 < devices, starts_ref[jnp.minimum(me + 1, devices - 1)], total)
    for s in range(held_kind.shape[0]):
        owner = owners_ref[jnp.minimum(start + s, total - 1)]
        held_kind[s] = jnp.where(start + s < end, partner_kind(me, owner), -1)


def tables(shard_starts, block_owners, me, slot_count, owned_slots):
    owned = jax.ShapeDtypeStruct((owned_slots,), jnp.int32)
    return pl.pallas_call(
        tables_kernel,
        in_specs=[pl.BlockSpec(memory_space=pltpu.SMEM)] * 3,
        out_specs=[pl.BlockSpec(memory_space=pltpu.SMEM)] * 3,
        out_shape=[owned, owned, jax.ShapeDtypeStruct((slot_count,), jnp.int32)],
        compiler_params=pltpu.CompilerParams(vmem_limit_bytes=SMALL_VMEM),
        name="tables",
    )(me.reshape(1), *in_hbm(shard_starts, block_owners))


def split(value):
    high = value.astype(jnp.bfloat16)
    return high, (value - high.astype(jnp.float32)).astype(jnp.bfloat16)


def product(a, b, dims):
    return lax.dot_general(a, b, (dims, ((), ())), preferred_element_type=jnp.float32)


def product3(a, b, dims):
    left = jnp.concatenate((a[0], a[0], a[1]), axis=dims[0][0])
    right = jnp.concatenate((b[0], b[1], b[0]), axis=dims[1][0])
    return product(left, right, dims)


NN = ((1,), (0,))
NT = ((1,), (1,))


def prepare_kernel(place_ref, moment_ref, second_ref, left_ref, right_ref, *outs):
    turned_out, second_out, flip_high, flip_low, right_high, right_low, row_high, row_low = outs
    every = range(moment_ref.shape[0])
    half = row_high.shape[1]
    here = pl.multiple_of(place_ref[0] * half, half)
    right = [split(right_ref[g]) for g in every]
    first = [product3(split(moment_ref[g]), right[g], NN) for g in every]
    flipped = [split(left_ref[g].T) for g in every]
    turned = [product3(flipped[g], split(first[g]), NN) for g in every]
    for g in every:
        turned_out[g] = turned[g] * (beta_one / bias_one)
        second_out[g] = second_ref[g] * beta_two
        flip_high[g], flip_low[g] = flipped[g]
        right_high[g], right_low[g] = right[g]
        row_high[g], row_low[g] = split(left_ref[g, pl.ds(here, half)])


def prepare(place, first_moment, second_moment, left_basis, right_basis, half):
    count, width, _ = first_moment.shape
    group = PREPARE_GROUP if count % PREPARE_GROUP == 0 else 1
    spec = pl.BlockSpec((group, width, width), lambda j: (j, 0, 0))
    part = pl.BlockSpec((group, half, width), lambda j: (j, 0, 0))
    full = pltpu.VMEM(first_moment.shape, jnp.float32)
    short = pltpu.VMEM(first_moment.shape, jnp.bfloat16)
    rows = pltpu.VMEM((count, half, width), jnp.bfloat16)
    return pl.pallas_call(
        prepare_kernel,
        grid=(count // group,),
        in_specs=[pl.BlockSpec(memory_space=pltpu.SMEM)] + [spec] * 4,
        out_specs=[spec] * 6 + [part] * 2,
        out_shape=[full] * 2 + [short] * 4 + [rows] * 2,
        compiler_params=pltpu.CompilerParams(vmem_limit_bytes=STEP_VMEM),
        cost_estimate=pl.CostEstimate(
            flops=12 * count * width**3, bytes_accessed=16 * count * width**2, transcendentals=0
        ),
        name="prepare",
    )(place, *in_hbm(first_moment, second_moment, left_basis, right_basis))


def load_kernel(place_ref, source_ref, out_ref):
    out_ref[...] = source_ref[...]


def load_rows(place, source, half):
    count, _, width = source.shape
    return pl.pallas_call(
        load_kernel,
        grid_spec=pltpu.PrefetchScalarGridSpec(
            num_scalar_prefetch=1,
            grid=(1,),
            in_specs=[pl.BlockSpec((count, half, width), lambda _, place: (0, place[0], 0))],
            out_specs=pl.BlockSpec((count, half, width), lambda _, place: (0, 0, 0)),
        ),
        out_shape=pltpu.VMEM((count, half, width), source.dtype),
        compiler_params=pltpu.CompilerParams(vmem_limit_bytes=SMALL_VMEM),
        name="load_rows",
    )(place, *in_hbm(source))


def add_kernel(place_ref, mine_ref, other_ref, out_ref):
    half = out_ref.shape[1]
    rows = pl.ds(pl.multiple_of(place_ref[0] * half, half), half)
    for s in range(out_ref.shape[0]):
        total = mine_ref[s].astype(jnp.float32) + other_ref[s, rows].astype(jnp.float32)
        out_ref[s] = total.astype(out_ref.dtype)


def add_replicas(place, mine, other):
    return pl.pallas_call(
        add_kernel,
        in_specs=[pl.BlockSpec(memory_space=pltpu.SMEM)]
        + [pl.BlockSpec(memory_space=pltpu.VMEM)] * 2,
        out_specs=pl.BlockSpec(memory_space=pltpu.VMEM),
        out_shape=pltpu.VMEM(mine.shape, mine.dtype),
        compiler_params=pltpu.CompilerParams(vmem_limit_bytes=SMALL_VMEM),
        name="add_replicas",
    )(place, *in_vmem(mine, other))


def collect_kernel(kind_ref, slot_ref, *refs):
    sources, out_ref = refs[:5], refs[5]
    for j in range(out_ref.shape[0]):
        for kind in range(5):

            @pl.when(kind_ref[j] == kind)
            def _():
                out_ref[j] = sources[kind][slot_ref[j]]


def collect(kind, slot, sources):
    count = kind.shape[0]
    return pl.pallas_call(
        collect_kernel,
        in_specs=[pl.BlockSpec(memory_space=pltpu.SMEM)] * 2
        + [pl.BlockSpec(memory_space=pltpu.VMEM)] * 5,
        out_specs=pl.BlockSpec(memory_space=pltpu.VMEM),
        out_shape=jax.ShapeDtypeStruct((count,) + sources[0].shape[1:], sources[0].dtype),
        compiler_params=pltpu.CompilerParams(vmem_limit_bytes=SMALL_VMEM),
        name="collect",
    )(kind, slot, *sources)


def step_kernel(kind_ref, slot_ref, place_ref, mine_ref, other_ref, *refs):
    turned_ref, second_ref, flip_high, flip_low, right_high, right_low, row_high, row_low = refs[:8]
    second_out, sends, codes, grads = refs[8], refs[9:14], refs[14], refs[15]
    step = pl.program_id(0)
    group, half = mine_ref.shape[:2]
    here = pl.multiple_of(place_ref[0] * half, half)
    there = pl.multiple_of((1 - place_ref[0]) * half, half)
    every = range(group)

    @pl.when(step == 0)
    def _():
        codes[...] = jnp.zeros_like(codes)

    for g in every:
        grads[g, pl.ds(here, half)] = mine_ref[g]
        grads[g, pl.ds(there, half)] = other_ref[g]
    right = [(right_high[g], right_low[g]) for g in every]
    first = [
        product(jnp.concatenate((grads[g],) * 2, axis=1), jnp.concatenate(right[g], axis=0), NN)
        for g in every
    ]
    turned = [product3((flip_high[g], flip_low[g]), split(first[g]), NN) for g in every]
    scaled = []
    for g in every:
        second = second_ref[g] + (1.0 - beta_two) * turned[g] * turned[g]
        second_out[g] = second
        unbiased = second * (1.0 / bias_two)
        root = unbiased * lax.rsqrt(unbiased)
        moment = turned_ref[g] + ((1.0 - beta_one) / bias_one) * turned[g]
        scaled.append(split(moment / (root + epsilon)))
    back = [product3((row_high[g], row_low[g]), scaled[g], NN) for g in every]
    update = [product3(split(back[g]), right[g], NT) for g in every]
    spots = lax.broadcasted_iota(jnp.int32, codes.shape[1:], 0)
    for g in every:
        peak = jnp.max(jnp.abs(update[g]), axis=0, keepdims=True)
        code = jnp.ceil(jnp.log2(jnp.maximum(peak, 1e-30) * (1.0 / 32000.0)) * CODE_STEPS)
        coded = jnp.round(update[g] * jnp.exp2(code * (-1.0 / CODE_STEPS)))
        coded = jnp.clip(coded, -32767.0, 32767.0).astype(jnp.int32).astype(jnp.int16)
        slot = slot_ref[step * group + g]
        rows = pl.ds(pl.multiple_of(slot * half, half), half)
        for kind in range(5):

            @pl.when(kind_ref[step * group + g] == kind)
            def _():
                sends[kind][rows] = coded
                codes[kind] = jnp.where(spots == slot, code.astype(jnp.int32), codes[kind])

    @pl.when(step == pl.num_programs(0) - 1)
    def _():
        for kind in range(5):
            top = sends[kind].shape[0] - CODE_ROWS
            sends[kind][pl.ds(top, CODE_ROWS)] = codes[kind].astype(jnp.int16)


def soap_step(kind, slot, place, mine, other, prepared, slot_count):
    count, half, width = mine.shape
    group = GROUP if count % GROUP == 0 else 1
    full = pl.BlockSpec((group, width, width), lambda j, *_: (j, 0, 0))
    part = pl.BlockSpec((group, half, width), lambda j, *_: (j, 0, 0))
    send_rows = slot_count * half + CODE_ROWS
    send = pl.BlockSpec((send_rows, width), lambda j, *_: (0, 0))
    return pl.pallas_call(
        step_kernel,
        grid_spec=pltpu.PrefetchScalarGridSpec(
            num_scalar_prefetch=3,
            grid=(count // group,),
            in_specs=[part, part] + [full] * 6 + [part] * 2,
            out_specs=[full] + [send] * 5,
            scratch_shapes=[
                pltpu.VMEM((5, CODE_ROWS, width), jnp.int32),
                pltpu.VMEM((group, width, width), jnp.bfloat16),
            ],
        ),
        out_shape=[pltpu.VMEM((count, width, width), jnp.float32)]
        + [pltpu.VMEM((send_rows, width), jnp.int16)] * 5,
        compiler_params=pltpu.CompilerParams(vmem_limit_bytes=STEP_VMEM),
        name="soap_step",
    )(kind, slot, place, *in_vmem(mine, other, *prepared))


def finish_kernel(kind_ref, place_ref, mine_ref, other_ref, moment_ref, second_ref, *outs):
    first_out, second_out = outs
    j = pl.program_id(0)
    half = mine_ref.shape[1]
    live = kind_ref[j] >= 0
    for place, part in ((place_ref[0], mine_ref), (1 - place_ref[0], other_ref)):
        rows = pl.ds(pl.multiple_of(place * half, half), half)
        gradient = part[0].astype(jnp.float32)
        moment = beta_one * moment_ref[0, rows] + (1.0 - beta_one) * gradient
        first_out[0, rows] = jnp.where(live, moment, 0.0)
    second_out[0] = jnp.where(live, second_ref[0], 0.0)


def finish(kind, place, mine, other, first_moment, second):
    count, width, _ = first_moment.shape
    half = mine.shape[1]
    full = pl.BlockSpec((1, width, width), lambda j: (j, 0, 0))
    part = pl.BlockSpec((1, half, width), lambda j: (j, 0, 0))
    return pl.pallas_call(
        finish_kernel,
        grid=(count,),
        in_specs=[pl.BlockSpec(memory_space=pltpu.SMEM)] * 2 + [part, part, full, full],
        out_specs=[full] * 2,
        out_shape=[pltpu.HBM(first_moment.shape, jnp.float32)] * 2,
        compiler_params=pltpu.CompilerParams(vmem_limit_bytes=SMALL_VMEM),
        cost_estimate=pl.CostEstimate(
            flops=12 * count * width**2, bytes_accessed=12 * count * width**2, transcendentals=0
        ),
        name="finish",
    )(kind, place, *in_vmem(mine, other), *in_hbm(first_moment), *in_vmem(second))


def gather_kernel(kind_ref, *refs):
    sources, out_ref = refs[:5], refs[5]
    count = kind_ref.shape[0]
    top = out_ref.shape[0] - CODE_ROWS
    half = top // count
    spots = lax.broadcasted_iota(jnp.int32, (CODE_ROWS, out_ref.shape[1]), 0)
    chosen = jnp.zeros(spots.shape, jnp.int32)
    for s in range(count):
        for kind in range(5):

            @pl.when(kind_ref[s] == kind)
            def _():
                rows = pl.ds(s * half, half)
                out_ref[rows] = sources[kind][rows]

    for kind in range(5):
        code = sources[kind][pl.ds(top, CODE_ROWS)].astype(jnp.int32)
        for s in range(count):
            chosen = jnp.where((spots == s) & (kind_ref[s] == kind), code, chosen)
    out_ref[pl.ds(top, CODE_ROWS)] = chosen.astype(jnp.int16)


def gather_held(kind, sources):
    return pl.pallas_call(
        gather_kernel,
        in_specs=[pl.BlockSpec(memory_space=pltpu.SMEM)]
        + [pl.BlockSpec(memory_space=pltpu.VMEM)] * 5,
        out_specs=pl.BlockSpec(memory_space=pltpu.VMEM),
        out_shape=jax.ShapeDtypeStruct(sources[0].shape, sources[0].dtype),
        compiler_params=pltpu.CompilerParams(vmem_limit_bytes=SMALL_VMEM),
        name="gather_held",
    )(kind, *sources)


def decode_kernel(kind_ref, place_ref, mine_ref, other_ref, out_ref, values, sems):
    count = values.shape[0]
    top = mine_ref.shape[0] - CODE_ROWS
    half = top // count
    both = ((place_ref[0], mine_ref), (1 - place_ref[0], other_ref))
    scales = []
    for _, coded in both:
        code = coded[pl.ds(top, CODE_ROWS)].astype(jnp.int32).astype(jnp.float32)
        scales.append(jnp.exp2(code * (1.0 / CODE_STEPS)))
    copies = []
    for s in range(count):
        for (place, coded), scale in zip(both, scales):
            value = coded[pl.ds(s * half, half)].astype(jnp.int32).astype(jnp.float32)
            to = pl.ds(pl.multiple_of(place * half, half), half)
            values[s, to] = jnp.where(kind_ref[s] >= 0, value * scale[s : s + 1], 0.0)
        copies.append(pltpu.make_async_copy(values.at[s], out_ref.at[s], sems.at[s]))
        copies[-1].start()
    for copy in copies:
        copy.wait()


def decode(kind, place, mine, other, width):
    count = kind.shape[0]
    return pl.pallas_call(
        decode_kernel,
        in_specs=[pl.BlockSpec(memory_space=pltpu.SMEM)] * 2
        + [pl.BlockSpec(memory_space=pltpu.VMEM)] * 2,
        out_specs=pl.BlockSpec(memory_space=pltpu.HBM),
        out_shape=pltpu.HBM((count, width, width), jnp.float32),
        scratch_shapes=[
            pltpu.VMEM((count, width, width), jnp.float32),
            pltpu.SemaphoreType.DMA((count,)),
        ],
        compiler_params=pltpu.CompilerParams(vmem_limit_bytes=SMALL_VMEM),
        name="decode",
    )(kind, place, mine, other)


def body(
    gradients, first_moment, second_moment, left_basis, right_basis, shard_starts, block_owners
):
    me = lax.axis_index("fsdp").astype(jnp.int32)
    core = lax.axis_index("dp").astype(jnp.int32)
    devices = lax.axis_size("fsdp")
    slot_count, width = gradients.shape[1], gradients.shape[3]
    owned_slots = first_moment.shape[0]
    half = width // lax.axis_size("dp")
    side, cross, flip, far = partner_pairs(devices)
    place = core.reshape(1)

    own_kind, own_slot, held_kind = tables(
        shard_starts, block_owners, me, slot_count, owned_slots
    )
    replica = gradients[0]
    twin = swap_cores(replica)

    summed = add_replicas(place, load_rows(place, replica, half), twin)
    by_flip = exchange(summed, flip)
    by_cross = exchange(summed, cross)
    by_far = exchange(summed, far)
    by_side = exchange(summed, side)
    prepared = prepare(place, first_moment, second_moment, left_basis, right_basis, half)
    mine = collect(own_kind, own_slot, (summed, by_side, by_cross, by_flip, by_far))
    other = swap_cores(mine)
    second, keep, to_side, to_cross, to_flip, to_far = soap_step(
        own_kind, own_slot, place, mine, other, prepared, slot_count
    )
    first_new, second_new = finish(own_kind, place, mine, other, first_moment, second)
    sent = (
        keep,
        exchange(to_side, side),
        exchange(to_cross, cross),
        exchange(to_flip, flip),
        exchange(to_far, far),
    )
    coded = gather_held(held_kind, sent)
    direction = decode(held_kind, place, coded, swap_cores(coded), width)
    return (direction, first_new, second_new)


def solution(mesh):
    in_specs = (
        P("dp", "fsdp", None, None),
        P("fsdp", None, None),
        P("fsdp", None, None),
        P("fsdp", None, None),
        P("fsdp", None, None),
        P(),
        P(),
    )
    out_specs = (P("fsdp", None, None), P("fsdp", None, None), P("fsdp", None, None))
    return jax.shard_map(body, mesh=mesh, in_specs=in_specs, out_specs=out_specs, check_vma=False)
```

```python
import functools

import jax
import jax.numpy as jnp
from jax import lax
from jax.experimental import pallas as pl
from jax.experimental.pallas import tpu as pltpu
from jax.sharding import PartitionSpec as P


REACH = 2
STEP = 10
CODE_ROWS = 8
CODE_STEPS = 128.0
PREPARE_GROUP = 3
GROUP = 6
SMALL_VMEM = 12 * 2**20
STEP_VMEM = 28 * 2**20

beta_one = 0.9
beta_two = 0.95
epsilon = 1e-08
bias_one = 1.0 - beta_one**STEP
bias_two = 1.0 - beta_two**STEP

HERE, SIDE, CROSS, FLIP, FAR = range(5)


def exchange(value, pairs):
    return lax.ppermute(value, "fsdp", pairs + [(b, a) for a, b in pairs])


def partner_pairs(devices):
    side = [(i, i + 1) for i in range(0, devices - 1, 2)]
    cross = [(i, i + 1) for i in range(1, devices - 1, 2)]
    flip = [(i, i + 2) for i in range(devices - 2) if not i & 2]
    far = [(i, i + 2) for i in range(devices - 2) if i & 2]
    return (side, cross, flip, far)


def swap_cores(value):
    return lax.ppermute(value, "dp", [(0, 1), (1, 0)])


def partner_kind(me, other):
    step = jnp.abs(other - me)
    near = jnp.where(other == me ^ 1, SIDE, CROSS)
    distant = jnp.where(other == me ^ 2, FLIP, FAR)
    return jnp.where(step == 0, HERE, jnp.where(step == 1, near, distant))


def in_hbm(*values):
    return tuple(pltpu.with_memory_space_constraint(value, pltpu.HBM) for value in values)


def in_vmem(*values):
    return tuple(pltpu.with_memory_space_constraint(value, pltpu.VMEM) for value in values)


def in_smem(*values):
    return tuple(pltpu.with_memory_space_constraint(value, pltpu.SMEM) for value in values)


def tables_kernel(at_ref, starts_ref, owners_ref, owned_kind, owned_slot, held_kind, core):
    me = at_ref[0]
    core[0] = at_ref[1]
    devices, total = starts_ref.shape[0], owners_ref.shape[0]

    def tally(b, sums):
        owner = owners_ref[b]
        return sums[0] + (owner < me).astype(jnp.int32), sums[1] + (owner == me).astype(jnp.int32)

    zero = jnp.int32(0)
    first, count = lax.fori_loop(0, total, tally, (zero, zero))
    near = [me + step for step in range(-REACH, REACH + 1)]
    begins = [starts_ref[jnp.clip(device, 0, devices - 1)] for device in near]
    for j in range(owned_kind.shape[0]):
        holder, start = near[0], begins[0]
        for device, begin in zip(near, begins):
            reached = (device >= 0) & (device < devices) & (begin <= first + j)
            holder = jnp.where(reached, device, holder)
            start = jnp.where(reached, begin, start)
        owned_kind[j] = jnp.where(j < count, partner_kind(me, holder), -1)
        owned_slot[j] = jnp.clip(first + j - start, 0, held_kind.shape[0] - 1)
    start = starts_ref[me]
    end = jnp.where(me + 1 < devices, starts_ref[jnp.minimum(me + 1, devices - 1)], total)
    for s in range(held_kind.shape[0]):
        owner = owners_ref[jnp.minimum(start + s, total - 1)]
        held_kind[s] = jnp.where(start + s < end, partner_kind(me, owner), -1)


def tables(shard_starts, block_owners, at, slot_count, owned_slots):
    owned = pltpu.SMEM((owned_slots,), jnp.int32)
    return pl.pallas_call(
        tables_kernel,
        in_specs=[pl.BlockSpec(memory_space=pltpu.SMEM)] * 3,
        out_specs=[pl.BlockSpec(memory_space=pltpu.SMEM)] * 4,
        out_shape=[owned, owned]
        + [pltpu.SMEM((size,), jnp.int32) for size in (slot_count, 1)],
        compiler_params=pltpu.CompilerParams(vmem_limit_bytes=SMALL_VMEM),
        name="tables",
    )(at, *in_hbm(shard_starts, block_owners))


def split(value):
    high = value.astype(jnp.bfloat16)
    return high, (value - high.astype(jnp.float32)).astype(jnp.bfloat16)


def product(a, b, dims):
    return lax.dot_general(a, b, (dims, ((), ())), preferred_element_type=jnp.float32)


def product3(a, b, dims):
    count = a[0].shape[0]
    tall = product(jnp.concatenate(a, axis=0), b[0], dims)
    return tall[:count] + (tall[count:] + product(a[0], b[1], dims))


NN = ((1,), (0,))
NT = ((1,), (1,))


def prepare_kernel(place_ref, moment_ref, second_ref, left_ref, right_ref, *outs):
    turned_out, second_out, flip_high, flip_low, right_high, right_low, row_high, row_low = outs
    every = range(moment_ref.shape[0])
    half = row_high.shape[1]
    here = pl.multiple_of(place_ref[0] * half, half)
    right = [split(right_ref[g]) for g in every]
    first = [product3(split(moment_ref[g]), right[g], NN) for g in every]
    flipped = [split(left_ref[g].T) for g in every]
    turned = [product3(flipped[g], split(first[g]), NN) for g in every]
    for g in every:
        turned_out[g] = turned[g] * (beta_one / bias_one)
        second_out[g] = second_ref[g] * beta_two
        flip_high[g], flip_low[g] = flipped[g]
        right_high[g], right_low[g] = right[g]
        row_high[g], row_low[g] = split(left_ref[g, pl.ds(here, half)])


def prepare(place, first_moment, second_moment, left_basis, right_basis, half):
    count, width, _ = first_moment.shape
    group = PREPARE_GROUP if count % PREPARE_GROUP == 0 else 1
    spec = pl.BlockSpec((group, width, width), lambda j: (j, 0, 0))
    part = pl.BlockSpec((group, half, width), lambda j: (j, 0, 0))
    full = pltpu.VMEM(first_moment.shape, jnp.float32)
    short = pltpu.VMEM(first_moment.shape, jnp.bfloat16)
    rows = pltpu.VMEM((count, half, width), jnp.bfloat16)
    return pl.pallas_call(
        prepare_kernel,
        grid=(count // group,),
        in_specs=[pl.BlockSpec(memory_space=pltpu.SMEM)] + [spec] * 4,
        out_specs=[spec] * 6 + [part] * 2,
        out_shape=[full] * 2 + [short] * 4 + [rows] * 2,
        compiler_params=pltpu.CompilerParams(vmem_limit_bytes=STEP_VMEM),
        cost_estimate=pl.CostEstimate(
            flops=12 * count * width**3, bytes_accessed=16 * count * width**2, transcendentals=0
        ),
        name="prepare",
    )(place, *in_hbm(first_moment, second_moment, left_basis, right_basis))


def load_kernel(place_ref, source_ref, out_ref):
    out_ref[...] = source_ref[...]


def load_rows(place, source, half):
    count, _, width = source.shape
    return pl.pallas_call(
        load_kernel,
        grid_spec=pltpu.PrefetchScalarGridSpec(
            num_scalar_prefetch=1,
            grid=(1,),
            in_specs=[pl.BlockSpec((count, half, width), lambda _, place: (0, place[0], 0))],
            out_specs=pl.BlockSpec((count, half, width), lambda _, place: (0, 0, 0)),
        ),
        out_shape=pltpu.VMEM((count, half, width), source.dtype),
        compiler_params=pltpu.CompilerParams(vmem_limit_bytes=SMALL_VMEM),
        name="load_rows",
    )(place, *in_hbm(source))


def add_kernel(place_ref, mine_ref, other_ref, out_ref):
    half = out_ref.shape[1]
    rows = pl.ds(pl.multiple_of(place_ref[0] * half, half), half)
    for s in range(out_ref.shape[0]):
        total = mine_ref[s].astype(jnp.float32) + other_ref[s, rows].astype(jnp.float32)
        out_ref[s] = total.astype(out_ref.dtype)


def add_replicas(place, mine, other):
    return pl.pallas_call(
        add_kernel,
        in_specs=[pl.BlockSpec(memory_space=pltpu.SMEM)]
        + [pl.BlockSpec(memory_space=pltpu.VMEM)] * 2,
        out_specs=pl.BlockSpec(memory_space=pltpu.VMEM),
        out_shape=pltpu.VMEM(mine.shape, mine.dtype),
        compiler_params=pltpu.CompilerParams(vmem_limit_bytes=SMALL_VMEM),
        name="add_replicas",
    )(place, *in_vmem(mine, other))


def collect_kernel(kind_ref, slot_ref, *refs):
    sources, out_ref = refs[:5], refs[5]
    for j in range(out_ref.shape[0]):
        for kind in range(5):

            @pl.when(kind_ref[j] == kind)
            def _():
                out_ref[j] = sources[kind][slot_ref[j]]


def collect(kind, slot, sources):
    count = kind.shape[0]
    return pl.pallas_call(
        collect_kernel,
        in_specs=[pl.BlockSpec(memory_space=pltpu.SMEM)] * 2
        + [pl.BlockSpec(memory_space=pltpu.VMEM)] * 5,
        out_specs=pl.BlockSpec(memory_space=pltpu.VMEM),
        out_shape=jax.ShapeDtypeStruct((count,) + sources[0].shape[1:], sources[0].dtype),
        compiler_params=pltpu.CompilerParams(vmem_limit_bytes=SMALL_VMEM),
        name="collect",
    )(*in_smem(kind, slot), *sources)


def step_kernel(kind_ref, slot_ref, place_ref, mine_ref, other_ref, *refs):
    turned_ref, second_ref, flip_high, flip_low, right_high, right_low, row_high, row_low = refs[:8]
    second_out, sends, codes, grads = refs[8], refs[9:14], refs[14], refs[15]
    step = pl.program_id(0)
    group, half = mine_ref.shape[:2]
    here = pl.multiple_of(place_ref[0] * half, half)
    there = pl.multiple_of((1 - place_ref[0]) * half, half)
    every = range(group)

    @pl.when(step == 0)
    def _():
        codes[...] = jnp.zeros_like(codes)

    spots = lax.broadcasted_iota(jnp.int32, codes.shape[1:], 0)
    at = [dict() for _ in every]

    def rotate_right(g):
        grads[g, pl.ds(here, half)] = mine_ref[g]
        grads[g, pl.ds(there, half)] = other_ref[g]
        wide = jnp.concatenate((grads[g],) * 2, axis=1)
        at[g]["first"] = product(wide, jnp.concatenate((right_high[g], right_low[g]), axis=0), NN)

    def rotate_left(g):
        at[g]["turned"] = product3((flip_high[g], flip_low[g]), split(at[g].pop("first")), NN)

    def scale(g):
        turned = at[g].pop("turned")
        second = second_ref[g] + (1.0 - beta_two) * turned * turned
        second_out[g] = second
        unbiased = second * (1.0 / bias_two)
        root = unbiased * lax.rsqrt(unbiased)
        moment = turned_ref[g] + ((1.0 - beta_one) / bias_one) * turned
        at[g]["scaled"] = split(moment / (root + epsilon))

    def return_left(g):
        at[g]["back"] = product3((row_high[g], row_low[g]), at[g].pop("scaled"), NN)

    def return_right(g):
        at[g]["update"] = product3(split(at[g].pop("back")), (right_high[g], right_low[g]), NT)

    def code_update(g):
        update = at[g].pop("update")
        peak = jnp.max(jnp.abs(update), axis=0, keepdims=True)
        code = jnp.ceil(jnp.log2(jnp.maximum(peak, 1e-30) * (1.0 / 32000.0)) * CODE_STEPS)
        coded = jnp.round(update * jnp.exp2(code * (-1.0 / CODE_STEPS)))
        coded = jnp.clip(coded, -32767.0, 32767.0).astype(jnp.int32).astype(jnp.int16)
        slot = slot_ref[step * group + g]
        rows = pl.ds(pl.multiple_of(slot * half, half), half)
        for kind in range(5):

            @pl.when(kind_ref[step * group + g] == kind)
            def _():
                sends[kind][rows] = coded
                codes[kind] = jnp.where(spots == slot, code.astype(jnp.int32), codes[kind])

    stages = (rotate_right, rotate_left, scale, return_left, return_right)
    for wave in range(group + len(stages) - 1):
        for depth in reversed(range(len(stages))):
            if 0 <= wave - depth < group:
                stages[depth](wave - depth)
    for g in every:
        code_update(g)

    @pl.when(step == pl.num_programs(0) - 1)
    def _():
        for kind in range(5):
            top = sends[kind].shape[0] - CODE_ROWS
            sends[kind][pl.ds(top, CODE_ROWS)] = codes[kind].astype(jnp.int16)


def soap_step(kind, slot, place, mine, other, prepared, slot_count):
    count, half, width = mine.shape
    group = GROUP if count % GROUP == 0 else 1
    full = pl.BlockSpec((group, width, width), lambda j: (j, 0, 0))
    part = pl.BlockSpec((group, half, width), lambda j: (j, 0, 0))
    send_rows = slot_count * half + CODE_ROWS
    send = pl.BlockSpec((send_rows, width), lambda j: (0, 0))
    return pl.pallas_call(
        step_kernel,
        grid=(count // group,),
        in_specs=[pl.BlockSpec(memory_space=pltpu.SMEM)] * 3
        + [part, part]
        + [full] * 6
        + [part] * 2,
        out_specs=[full] + [send] * 5,
        scratch_shapes=[
            pltpu.VMEM((5, CODE_ROWS, width), jnp.int32),
            pltpu.VMEM((group, width, width), jnp.bfloat16),
        ],
        out_shape=[pltpu.VMEM((count, width, width), jnp.float32)]
        + [pltpu.VMEM((send_rows, width), jnp.int16)] * 5,
        compiler_params=pltpu.CompilerParams(vmem_limit_bytes=STEP_VMEM),
        name="soap_step",
    )(*in_smem(kind, slot, place), *in_vmem(mine, other, *prepared))


def finish_kernel(kind_ref, place_ref, mine_ref, other_ref, moment_ref, second_ref, *outs):
    first_out, second_out = outs
    j = pl.program_id(0)
    half = mine_ref.shape[1]
    live = kind_ref[j] >= 0
    for place, part in ((place_ref[0], mine_ref), (1 - place_ref[0], other_ref)):
        rows = pl.ds(pl.multiple_of(place * half, half), half)
        gradient = part[0].astype(jnp.float32)
        moment = beta_one * moment_ref[0, rows] + (1.0 - beta_one) * gradient
        first_out[0, rows] = jnp.where(live, moment, 0.0)
    second_out[0] = jnp.where(live, second_ref[0], 0.0)


def finish(kind, place, mine, other, first_moment, second):
    count, width, _ = first_moment.shape
    half = mine.shape[1]
    full = pl.BlockSpec((1, width, width), lambda j: (j, 0, 0))
    part = pl.BlockSpec((1, half, width), lambda j: (j, 0, 0))
    return pl.pallas_call(
        finish_kernel,
        grid=(count,),
        in_specs=[pl.BlockSpec(memory_space=pltpu.SMEM)] * 2 + [part, part, full, full],
        out_specs=[full] * 2,
        out_shape=[pltpu.HBM(first_moment.shape, jnp.float32)] * 2,
        compiler_params=pltpu.CompilerParams(vmem_limit_bytes=SMALL_VMEM),
        cost_estimate=pl.CostEstimate(
            flops=12 * count * width**2, bytes_accessed=12 * count * width**2, transcendentals=0
        ),
        name="finish",
    )(*in_smem(kind, place), *in_vmem(mine, other), *in_hbm(first_moment), *in_vmem(second))


def gather_kernel(kind_ref, *refs):
    sources, out_ref = refs[:5], refs[5]
    count = kind_ref.shape[0]
    top = out_ref.shape[0] - CODE_ROWS
    half = top // count
    spots = lax.broadcasted_iota(jnp.int32, (CODE_ROWS, out_ref.shape[1]), 0)
    chosen = jnp.zeros(spots.shape, jnp.int32)
    for s in range(count):
        for kind in range(5):

            @pl.when(kind_ref[s] == kind)
            def _():
                rows = pl.ds(s * half, half)
                out_ref[rows] = sources[kind][rows]

    for kind in range(5):
        code = sources[kind][pl.ds(top, CODE_ROWS)].astype(jnp.int32)
        for s in range(count):
            chosen = jnp.where((spots == s) & (kind_ref[s] == kind), code, chosen)
    out_ref[pl.ds(top, CODE_ROWS)] = chosen.astype(jnp.int16)


def gather_held(kind, sources):
    return pl.pallas_call(
        gather_kernel,
        in_specs=[pl.BlockSpec(memory_space=pltpu.SMEM)]
        + [pl.BlockSpec(memory_space=pltpu.VMEM)] * 5,
        out_specs=pl.BlockSpec(memory_space=pltpu.VMEM),
        out_shape=jax.ShapeDtypeStruct(sources[0].shape, sources[0].dtype),
        compiler_params=pltpu.CompilerParams(vmem_limit_bytes=SMALL_VMEM),
        name="gather_held",
    )(*in_smem(kind), *sources)


def decode_kernel(kind_ref, core_ref, coded_ref, *refs, twin):
    out_ref, values, sems = refs[-3:]
    count, half = values.shape[:2]
    top = count * half
    place = 1 - core_ref[0] if twin else core_ref[0]
    to = pl.ds(pl.multiple_of(place * half, half), half)
    code = coded_ref[pl.ds(top, CODE_ROWS)].astype(jnp.int32).astype(jnp.float32)
    scales = jnp.exp2(code * (1.0 / CODE_STEPS))
    copies = []
    for s in range(count):
        value = coded_ref[pl.ds(s * half, half)].astype(jnp.int32).astype(jnp.float32)
        values[s] = jnp.where(kind_ref[s] >= 0, value * scales[s : s + 1], 0.0)
        copies.append(pltpu.make_async_copy(values.at[s], out_ref.at[s, to], sems.at[s]))
        copies[-1].start()
    for copy in copies:
        copy.wait()


def decode(kind, core, coded, base, width):
    count = kind.shape[0]
    half = (coded.shape[0] - CODE_ROWS) // count
    twin = base is not None
    return pl.pallas_call(
        functools.partial(decode_kernel, twin=twin),
        in_specs=[pl.BlockSpec(memory_space=pltpu.SMEM)] * 2
        + [pl.BlockSpec(memory_space=pltpu.VMEM)]
        + [pl.BlockSpec(memory_space=pltpu.HBM)] * twin,
        out_specs=pl.BlockSpec(memory_space=pltpu.HBM),
        out_shape=pltpu.HBM((count, width, width), jnp.float32),
        input_output_aliases={3: 0} if twin else {},
        scratch_shapes=[
            pltpu.VMEM((count, half, width), jnp.float32),
            pltpu.SemaphoreType.DMA((count,)),
        ],
        compiler_params=pltpu.CompilerParams(vmem_limit_bytes=SMALL_VMEM),
        cost_estimate=pl.CostEstimate(
            flops=count * half * width, bytes_accessed=6 * count * half * width, transcendentals=0
        ),
        name="decode_twin" if twin else "decode_own",
    )(*in_smem(kind, core), coded, *((base,) if twin else ()))


def body(
    gradients, first_moment, second_moment, left_basis, right_basis, shard_starts, block_owners
):
    me = lax.axis_index("fsdp").astype(jnp.int32)
    core = lax.axis_index("dp").astype(jnp.int32)
    devices = lax.axis_size("fsdp")
    slot_count, width = gradients.shape[1], gradients.shape[3]
    owned_slots = first_moment.shape[0]
    half = width // lax.axis_size("dp")
    side, cross, flip, far = partner_pairs(devices)
    place = core.reshape(1)

    own_kind, own_slot, held_kind, core_index = tables(
        shard_starts, block_owners, jnp.stack((me, core)), slot_count, owned_slots
    )
    replica = gradients[0]
    twin = swap_cores(replica)

    summed = add_replicas(place, load_rows(place, replica, half), twin)
    by_flip = exchange(summed, flip)
    by_cross = exchange(summed, cross)
    by_far = exchange(summed, far)
    by_side = exchange(summed, side)
    prepared = prepare(place, first_moment, second_moment, left_basis, right_basis, half)
    mine = collect(own_kind, own_slot, (summed, by_side, by_cross, by_flip, by_far))
    other = swap_cores(mine)
    second, keep, to_side, to_cross, to_flip, to_far = soap_step(
        own_kind, own_slot, core_index, mine, other, prepared, slot_count
    )
    first_new, second_new = finish(own_kind, core_index, mine, other, first_moment, second)
    sent = (
        keep,
        exchange(to_side, side),
        exchange(to_cross, cross),
        exchange(to_flip, flip),
        exchange(to_far, far),
    )
    coded = gather_held(held_kind, sent)
    twin_coded = swap_cores(coded)
    direction = decode(held_kind, core_index, coded, None, width)
    direction = decode(held_kind, core_index, twin_coded, direction, width)
    return (direction, first_new, second_new)


def solution(mesh):
    in_specs = (
        P("dp", "fsdp", None, None),
        P("fsdp", None, None),
        P("fsdp", None, None),
        P("fsdp", None, None),
        P("fsdp", None, None),
        P(),
        P(),
    )
    out_specs = (P("fsdp", None, None), P("fsdp", None, None), P("fsdp", None, None))
    return jax.shard_map(body, mesh=mesh, in_specs=in_specs, out_specs=out_specs, check_vma=False)
```

```python
import functools

import jax
import jax.numpy as jnp
from jax import lax
from jax.experimental import pallas as pl
from jax.experimental.pallas import tpu as pltpu
from jax.sharding import PartitionSpec as P


REACH = 2
STEP = 10
CODE_ROWS = 8
CODE_STEPS = 128.0
PREPARE_GROUP = 3
GROUP = 6
SMALL_VMEM = 12 * 2**20
STEP_VMEM = 28 * 2**20

beta_one = 0.9
beta_two = 0.95
epsilon = 1e-08
bias_one = 1.0 - beta_one**STEP
bias_two = 1.0 - beta_two**STEP

HERE, SIDE, CROSS, FLIP, FAR = range(5)


def exchange(value, pairs):
    return lax.ppermute(value, "fsdp", pairs + [(b, a) for a, b in pairs])


def partner_pairs(devices):
    side = [(i, i + 1) for i in range(0, devices - 1, 2)]
    cross = [(i, i + 1) for i in range(1, devices - 1, 2)]
    flip = [(i, i + 2) for i in range(devices - 2) if not i & 2]
    far = [(i, i + 2) for i in range(devices - 2) if i & 2]
    return (side, cross, flip, far)


def swap_cores(value):
    return lax.ppermute(value, "dp", [(0, 1), (1, 0)])


def partner_kind(me, other):
    step = jnp.abs(other - me)
    near = jnp.where(other == me ^ 1, SIDE, CROSS)
    distant = jnp.where(other == me ^ 2, FLIP, FAR)
    return jnp.where(step == 0, HERE, jnp.where(step == 1, near, distant))


def in_hbm(*values):
    return tuple(pltpu.with_memory_space_constraint(value, pltpu.HBM) for value in values)


def in_vmem(*values):
    return tuple(pltpu.with_memory_space_constraint(value, pltpu.VMEM) for value in values)


def in_smem(*values):
    return tuple(pltpu.with_memory_space_constraint(value, pltpu.SMEM) for value in values)


def tables_kernel(at_ref, starts_ref, owners_ref, owned_kind, owned_slot, held_kind, core):
    me = at_ref[0]
    core[0] = at_ref[1]
    devices, total = starts_ref.shape[0], owners_ref.shape[0]

    def tally(b, sums):
        owner = owners_ref[b]
        return sums[0] + (owner < me).astype(jnp.int32), sums[1] + (owner == me).astype(jnp.int32)

    zero = jnp.int32(0)
    first, count = lax.fori_loop(0, total, tally, (zero, zero))
    near = [me + step for step in range(-REACH, REACH + 1)]
    begins = [starts_ref[jnp.clip(device, 0, devices - 1)] for device in near]
    for j in range(owned_kind.shape[0]):
        holder, start = near[0], begins[0]
        for device, begin in zip(near, begins):
            reached = (device >= 0) & (device < devices) & (begin <= first + j)
            holder = jnp.where(reached, device, holder)
            start = jnp.where(reached, begin, start)
        owned_kind[j] = jnp.where(j < count, partner_kind(me, holder), -1)
        owned_slot[j] = jnp.clip(first + j - start, 0, held_kind.shape[0] - 1)
    start = starts_ref[me]
    end = jnp.where(me + 1 < devices, starts_ref[jnp.minimum(me + 1, devices - 1)], total)
    for s in range(held_kind.shape[0]):
        owner = owners_ref[jnp.minimum(start + s, total - 1)]
        held_kind[s] = jnp.where(start + s < end, partner_kind(me, owner), -1)


def tables(shard_starts, block_owners, at, slot_count, owned_slots):
    owned = pltpu.SMEM((owned_slots,), jnp.int32)
    return pl.pallas_call(
        tables_kernel,
        in_specs=[pl.BlockSpec(memory_space=pltpu.SMEM)] * 3,
        out_specs=[pl.BlockSpec(memory_space=pltpu.SMEM)] * 4,
        out_shape=[owned, owned]
        + [pltpu.SMEM((size,), jnp.int32) for size in (slot_count, 1)],
        compiler_params=pltpu.CompilerParams(vmem_limit_bytes=SMALL_VMEM),
        name="tables",
    )(at, *in_hbm(shard_starts, block_owners))


def split(value):
    high = value.astype(jnp.bfloat16)
    return high, (value - high.astype(jnp.float32)).astype(jnp.bfloat16)


def product(a, b, dims):
    return lax.dot_general(a, b, (dims, ((), ())), preferred_element_type=jnp.float32)


def product3(a, b, dims):
    count = a[0].shape[0]
    tall = product(jnp.concatenate(a, axis=0), b[0], dims)
    return tall[:count] + (tall[count:] + product(a[0], b[1], dims))


NN = ((1,), (0,))
NT = ((1,), (1,))


def prepare_kernel(place_ref, moment_ref, second_ref, left_ref, right_ref, *outs):
    turned_out, second_out, flip_high, flip_low, right_high, right_low, row_high, row_low = outs
    every = range(moment_ref.shape[0])
    half = row_high.shape[1]
    here = pl.multiple_of(place_ref[0] * half, half)
    right = [split(right_ref[g]) for g in every]
    first = [product3(split(moment_ref[g]), right[g], NN) for g in every]
    flipped = [split(left_ref[g].T) for g in every]
    turned = [product3(flipped[g], split(first[g]), NN) for g in every]
    for g in every:
        turned_out[g] = turned[g] * (beta_one / bias_one)
        second_out[g] = second_ref[g] * beta_two
        flip_high[g], flip_low[g] = flipped[g]
        right_high[g], right_low[g] = right[g]
        row_high[g], row_low[g] = split(left_ref[g, pl.ds(here, half)])


def prepare(place, first_moment, second_moment, left_basis, right_basis, half):
    count, width, _ = first_moment.shape
    group = PREPARE_GROUP if count % PREPARE_GROUP == 0 else 1
    spec = pl.BlockSpec((group, width, width), lambda j: (j, 0, 0))
    part = pl.BlockSpec((group, half, width), lambda j: (j, 0, 0))
    full = pltpu.VMEM(first_moment.shape, jnp.float32)
    short = pltpu.VMEM(first_moment.shape, jnp.bfloat16)
    rows = pltpu.VMEM((count, half, width), jnp.bfloat16)
    return pl.pallas_call(
        prepare_kernel,
        grid=(count // group,),
        in_specs=[pl.BlockSpec(memory_space=pltpu.SMEM)] + [spec] * 4,
        out_specs=[spec] * 6 + [part] * 2,
        out_shape=[full] * 2 + [short] * 4 + [rows] * 2,
        compiler_params=pltpu.CompilerParams(vmem_limit_bytes=STEP_VMEM),
        cost_estimate=pl.CostEstimate(
            flops=12 * count * width**3, bytes_accessed=16 * count * width**2, transcendentals=0
        ),
        name="prepare",
    )(place, *in_hbm(first_moment, second_moment, left_basis, right_basis))


def load_kernel(place_ref, source_ref, out_ref):
    out_ref[...] = source_ref[...]


def load_rows(place, source, half):
    count, _, width = source.shape
    return pl.pallas_call(
        load_kernel,
        grid_spec=pltpu.PrefetchScalarGridSpec(
            num_scalar_prefetch=1,
            grid=(1,),
            in_specs=[pl.BlockSpec((count, half, width), lambda _, place: (0, place[0], 0))],
            out_specs=pl.BlockSpec((count, half, width), lambda _, place: (0, 0, 0)),
        ),
        out_shape=pltpu.VMEM((count, half, width), source.dtype),
        compiler_params=pltpu.CompilerParams(vmem_limit_bytes=SMALL_VMEM),
        name="load_rows",
    )(place, *in_hbm(source))


def add_kernel(place_ref, mine_ref, other_ref, out_ref):
    half = out_ref.shape[1]
    rows = pl.ds(pl.multiple_of(place_ref[0] * half, half), half)
    for s in range(out_ref.shape[0]):
        total = mine_ref[s].astype(jnp.float32) + other_ref[s, rows].astype(jnp.float32)
        out_ref[s] = total.astype(out_ref.dtype)


def add_replicas(place, mine, other):
    return pl.pallas_call(
        add_kernel,
        in_specs=[pl.BlockSpec(memory_space=pltpu.SMEM)]
        + [pl.BlockSpec(memory_space=pltpu.VMEM)] * 2,
        out_specs=pl.BlockSpec(memory_space=pltpu.VMEM),
        out_shape=pltpu.VMEM(mine.shape, mine.dtype),
        compiler_params=pltpu.CompilerParams(vmem_limit_bytes=SMALL_VMEM),
        name="add_replicas",
    )(place, *in_vmem(mine, other))


def collect_kernel(kind_ref, slot_ref, *refs):
    sources, out_ref = refs[:5], refs[5]
    for j in range(out_ref.shape[0]):
        for kind in range(5):

            @pl.when(kind_ref[j] == kind)
            def _():
                out_ref[j] = sources[kind][slot_ref[j]]


def collect(kind, slot, sources):
    count = kind.shape[0]
    return pl.pallas_call(
        collect_kernel,
        in_specs=[pl.BlockSpec(memory_space=pltpu.SMEM)] * 2
        + [pl.BlockSpec(memory_space=pltpu.VMEM)] * 5,
        out_specs=pl.BlockSpec(memory_space=pltpu.VMEM),
        out_shape=jax.ShapeDtypeStruct((count,) + sources[0].shape[1:], sources[0].dtype),
        compiler_params=pltpu.CompilerParams(vmem_limit_bytes=SMALL_VMEM),
        name="collect",
    )(*in_smem(kind, slot), *sources)


def rotate_kernel(mine_ref, right_high, right_low, high_ref, low_ref):
    for g in range(mine_ref.shape[0]):
        gradient = mine_ref[g]
        turned = product(gradient, right_high[g], NN) + product(gradient, right_low[g], NN)
        high_ref[g], low_ref[g] = split(turned)


def rotate_rows(mine, prepared):
    right = prepared[4:6]
    return pl.pallas_call(
        rotate_kernel,
        in_specs=[pl.BlockSpec(memory_space=pltpu.VMEM)] * 3,
        out_specs=[pl.BlockSpec(memory_space=pltpu.VMEM)] * 2,
        out_shape=[pltpu.VMEM(mine.shape, jnp.bfloat16)] * 2,
        compiler_params=pltpu.CompilerParams(vmem_limit_bytes=SMALL_VMEM),
        cost_estimate=pl.CostEstimate(
            flops=4 * mine.size * mine.shape[2], bytes_accessed=6 * mine.size, transcendentals=0
        ),
        name="rotate_rows",
    )(*in_vmem(mine, *right))


def step_kernel(kind_ref, slot_ref, place_ref, mine_high, mine_low, other_ref, *refs):
    turned_ref, second_ref, flip_high, flip_low, right_high, right_low, row_high, row_low = refs[:8]
    second_out, sends, codes, first_high, first_low = refs[8], refs[9:14], *refs[14:]
    step = pl.program_id(0)
    group, half = other_ref.shape[:2]
    here = pl.multiple_of(place_ref[0] * half, half)
    there = pl.multiple_of((1 - place_ref[0]) * half, half)
    every = range(group)

    @pl.when(step == 0)
    def _():
        codes[...] = jnp.zeros_like(codes)

    spots = lax.broadcasted_iota(jnp.int32, codes.shape[1:], 0)
    at = [dict() for _ in every]

    def rotate_right(g):
        gradient = other_ref[g]
        turned = product(gradient, right_high[g], NN) + product(gradient, right_low[g], NN)
        high, low = split(turned)
        first_high[g, pl.ds(here, half)], first_low[g, pl.ds(here, half)] = mine_high[g], mine_low[g]
        first_high[g, pl.ds(there, half)], first_low[g, pl.ds(there, half)] = high, low

    def rotate_left(g):
        first = (first_high[g], first_low[g])
        at[g]["turned"] = product3((flip_high[g], flip_low[g]), first, NN)

    def scale(g):
        turned = at[g].pop("turned")
        second = second_ref[g] + (1.0 - beta_two) * turned * turned
        second_out[g] = second
        unbiased = second * (1.0 / bias_two)
        root = unbiased * lax.rsqrt(unbiased)
        moment = turned_ref[g] + ((1.0 - beta_one) / bias_one) * turned
        at[g]["scaled"] = split(moment / (root + epsilon))

    def return_left(g):
        at[g]["back"] = product3((row_high[g], row_low[g]), at[g].pop("scaled"), NN)

    def return_right(g):
        at[g]["update"] = product3(split(at[g].pop("back")), (right_high[g], right_low[g]), NT)

    def quantize(g):
        update = at[g].pop("update")
        peak = jnp.max(jnp.abs(update), axis=0, keepdims=True)
        code = jnp.ceil(jnp.log2(jnp.maximum(peak, 1e-30) * (1.0 / 32000.0)) * CODE_STEPS)
        coded = jnp.round(update * jnp.exp2(code * (-1.0 / CODE_STEPS)))
        at[g]["coded"] = jnp.clip(coded, -32767.0, 32767.0).astype(jnp.int32).astype(jnp.int16)
        at[g]["code"] = code.astype(jnp.int32)

    def deliver(g):
        coded, code = at[g].pop("coded"), at[g].pop("code")
        slot = slot_ref[step * group + g]
        rows = pl.ds(pl.multiple_of(slot * half, half), half)
        for kind in range(5):

            @pl.when(kind_ref[step * group + g] == kind)
            def _():
                sends[kind][rows] = coded
                codes[kind] = jnp.where(spots == slot, code, codes[kind])

    stages = (rotate_right, rotate_left, scale, return_left, return_right, quantize)
    for wave in range(group + len(stages) - 1):
        for depth in reversed(range(len(stages))):
            if 0 <= wave - depth < group:
                stages[depth](wave - depth)
    for g in every:
        deliver(g)

    @pl.when(step == pl.num_programs(0) - 1)
    def _():
        for kind in range(5):
            top = sends[kind].shape[0] - CODE_ROWS
            sends[kind][pl.ds(top, CODE_ROWS)] = codes[kind].astype(jnp.int16)


def soap_step(kind, slot, place, rotated, other, prepared, slot_count):
    count, half, width = other.shape
    group = GROUP if count % GROUP == 0 else 1
    full = pl.BlockSpec((group, width, width), lambda j: (j, 0, 0))
    part = pl.BlockSpec((group, half, width), lambda j: (j, 0, 0))
    send_rows = slot_count * half + CODE_ROWS
    send = pl.BlockSpec((send_rows, width), lambda j: (0, 0))
    return pl.pallas_call(
        step_kernel,
        grid=(count // group,),
        in_specs=[pl.BlockSpec(memory_space=pltpu.SMEM)] * 3
        + [part] * 3
        + [full] * 6
        + [part] * 2,
        out_specs=[full] + [send] * 5,
        scratch_shapes=[
            pltpu.VMEM((5, CODE_ROWS, width), jnp.int32),
            pltpu.VMEM((group, width, width), jnp.bfloat16),
            pltpu.VMEM((group, width, width), jnp.bfloat16),
        ],
        out_shape=[pltpu.VMEM((count, width, width), jnp.float32)]
        + [pltpu.VMEM((send_rows, width), jnp.int16)] * 5,
        compiler_params=pltpu.CompilerParams(vmem_limit_bytes=STEP_VMEM),
        name="soap_step",
    )(*in_smem(kind, slot, place), *in_vmem(*rotated, other, *prepared))


def finish_kernel(kind_ref, place_ref, mine_ref, other_ref, moment_ref, second_ref, *outs):
    first_out, second_out = outs
    j = pl.program_id(0)
    half = mine_ref.shape[1]
    live = kind_ref[j] >= 0
    for place, part in ((place_ref[0], mine_ref), (1 - place_ref[0], other_ref)):
        rows = pl.ds(pl.multiple_of(place * half, half), half)
        gradient = part[0].astype(jnp.float32)
        moment = beta_one * moment_ref[0, rows] + (1.0 - beta_one) * gradient
        first_out[0, rows] = jnp.where(live, moment, 0.0)
    second_out[0] = jnp.where(live, second_ref[0], 0.0)


def finish(kind, place, mine, other, first_moment, second):
    count, width, _ = first_moment.shape
    half = mine.shape[1]
    full = pl.BlockSpec((1, width, width), lambda j: (j, 0, 0))
    part = pl.BlockSpec((1, half, width), lambda j: (j, 0, 0))
    return pl.pallas_call(
        finish_kernel,
        grid=(count,),
        in_specs=[pl.BlockSpec(memory_space=pltpu.SMEM)] * 2 + [part, part, full, full],
        out_specs=[full] * 2,
        out_shape=[pltpu.HBM(first_moment.shape, jnp.float32)] * 2,
        compiler_params=pltpu.CompilerParams(vmem_limit_bytes=SMALL_VMEM),
        cost_estimate=pl.CostEstimate(
            flops=12 * count * width**2, bytes_accessed=12 * count * width**2, transcendentals=0
        ),
        name="finish",
    )(*in_smem(kind, place), *in_vmem(mine, other), *in_hbm(first_moment), *in_vmem(second))


def gather_kernel(kind_ref, *refs):
    sources, out_ref = refs[:5], refs[5]
    count = kind_ref.shape[0]
    top = out_ref.shape[0] - CODE_ROWS
    half = top // count
    spots = lax.broadcasted_iota(jnp.int32, (CODE_ROWS, out_ref.shape[1]), 0)
    chosen = jnp.zeros(spots.shape, jnp.int32)
    for s in range(count):
        for kind in range(5):

            @pl.when(kind_ref[s] == kind)
            def _():
                rows = pl.ds(s * half, half)
                out_ref[rows] = sources[kind][rows]

    for kind in range(5):
        code = sources[kind][pl.ds(top, CODE_ROWS)].astype(jnp.int32)
        for s in range(count):
            chosen = jnp.where((spots == s) & (kind_ref[s] == kind), code, chosen)
    out_ref[pl.ds(top, CODE_ROWS)] = chosen.astype(jnp.int16)


def gather_held(kind, sources):
    return pl.pallas_call(
        gather_kernel,
        in_specs=[pl.BlockSpec(memory_space=pltpu.SMEM)]
        + [pl.BlockSpec(memory_space=pltpu.VMEM)] * 5,
        out_specs=pl.BlockSpec(memory_space=pltpu.VMEM),
        out_shape=jax.ShapeDtypeStruct(sources[0].shape, sources[0].dtype),
        compiler_params=pltpu.CompilerParams(vmem_limit_bytes=SMALL_VMEM),
        name="gather_held",
    )(*in_smem(kind), *sources)


def decode_kernel(kind_ref, core_ref, coded_ref, *refs, twin):
    out_ref, values, sems = refs[-3:]
    count, half = values.shape[:2]
    top = count * half
    place = 1 - core_ref[0] if twin else core_ref[0]
    to = pl.ds(pl.multiple_of(place * half, half), half)
    code = coded_ref[pl.ds(top, CODE_ROWS)].astype(jnp.int32).astype(jnp.float32)
    scales = jnp.exp2(code * (1.0 / CODE_STEPS))
    copies = []
    for s in range(count):
        value = coded_ref[pl.ds(s * half, half)].astype(jnp.int32).astype(jnp.float32)
        values[s] = jnp.where(kind_ref[s] >= 0, value * scales[s : s + 1], 0.0)
        copies.append(pltpu.make_async_copy(values.at[s], out_ref.at[s, to], sems.at[s]))
        copies[-1].start()
    for copy in copies:
        copy.wait()


def decode(kind, core, coded, base, width):
    count = kind.shape[0]
    half = (coded.shape[0] - CODE_ROWS) // count
    twin = base is not None
    return pl.pallas_call(
        functools.partial(decode_kernel, twin=twin),
        in_specs=[pl.BlockSpec(memory_space=pltpu.SMEM)] * 2
        + [pl.BlockSpec(memory_space=pltpu.VMEM)]
        + [pl.BlockSpec(memory_space=pltpu.HBM)] * twin,
        out_specs=pl.BlockSpec(memory_space=pltpu.HBM),
        out_shape=pltpu.HBM((count, width, width), jnp.float32),
        input_output_aliases={3: 0} if twin else {},
        scratch_shapes=[
            pltpu.VMEM((count, half, width), jnp.float32),
            pltpu.SemaphoreType.DMA((count,)),
        ],
        compiler_params=pltpu.CompilerParams(vmem_limit_bytes=SMALL_VMEM),
        cost_estimate=pl.CostEstimate(
            flops=count * half * width, bytes_accessed=6 * count * half * width, transcendentals=0
        ),
        name="decode_twin" if twin else "decode_own",
    )(*in_smem(kind, core), coded, *((base,) if twin else ()))


def body(
    gradients, first_moment, second_moment, left_basis, right_basis, shard_starts, block_owners
):
    me = lax.axis_index("fsdp").astype(jnp.int32)
    core = lax.axis_index("dp").astype(jnp.int32)
    devices = lax.axis_size("fsdp")
    slot_count, width = gradients.shape[1], gradients.shape[3]
    owned_slots = first_moment.shape[0]
    half = width // lax.axis_size("dp")
    side, cross, flip, far = partner_pairs(devices)
    place = core.reshape(1)

    own_kind, own_slot, held_kind, core_index = tables(
        shard_starts, block_owners, jnp.stack((me, core)), slot_count, owned_slots
    )
    replica = gradients[0]
    twin = swap_cores(replica)

    summed = add_replicas(place, load_rows(place, replica, half), twin)
    by_flip = exchange(summed, flip)
    by_cross = exchange(summed, cross)
    by_far = exchange(summed, far)
    by_side = exchange(summed, side)
    prepared = prepare(place, first_moment, second_moment, left_basis, right_basis, half)
    mine = collect(own_kind, own_slot, (summed, by_side, by_cross, by_flip, by_far))
    other = swap_cores(mine)
    second, keep, to_side, to_cross, to_flip, to_far = soap_step(
        own_kind, own_slot, core_index, rotate_rows(mine, prepared), other, prepared, slot_count
    )
    first_new, second_new = finish(own_kind, core_index, mine, other, first_moment, second)
    sent = (
        keep,
        exchange(to_side, side),
        exchange(to_cross, cross),
        exchange(to_flip, flip),
        exchange(to_far, far),
    )
    coded = gather_held(held_kind, sent)
    twin_coded = swap_cores(coded)
    direction = decode(held_kind, core_index, coded, None, width)
    direction = decode(held_kind, core_index, twin_coded, direction, width)
    return (direction, first_new, second_new)


def solution(mesh):
    in_specs = (
        P("dp", "fsdp", None, None),
        P("fsdp", None, None),
        P("fsdp", None, None),
        P("fsdp", None, None),
        P("fsdp", None, None),
        P(),
        P(),
    )
    out_specs = (P("fsdp", None, None), P("fsdp", None, None), P("fsdp", None, None))
    return jax.shard_map(body, mesh=mesh, in_specs=in_specs, out_specs=out_specs, check_vma=False)
```

```python
import functools

import jax
import jax.numpy as jnp
from jax import lax
from jax.experimental import pallas as pl
from jax.experimental.pallas import tpu as pltpu
from jax.sharding import PartitionSpec as P


REACH = 2
STEP = 10
CODE_ROWS = 8
CODE_STEPS = 128.0
PREPARE_GROUP = 3
GROUP = 6
SMALL_VMEM = 12 * 2**20
STEP_VMEM = 28 * 2**20

beta_one = 0.9
beta_two = 0.95
epsilon = 1e-08
bias_one = 1.0 - beta_one**STEP
bias_two = 1.0 - beta_two**STEP

HERE, SIDE, CROSS, FLIP, FAR = range(5)


def exchange(value, pairs):
    return lax.ppermute(value, "fsdp", pairs + [(b, a) for a, b in pairs])


def partner_pairs(devices):
    side = [(i, i + 1) for i in range(0, devices - 1, 2)]
    cross = [(i, i + 1) for i in range(1, devices - 1, 2)]
    flip = [(i, i + 2) for i in range(devices - 2) if not i & 2]
    far = [(i, i + 2) for i in range(devices - 2) if i & 2]
    return (side, cross, flip, far)


def swap_cores(value):
    return lax.ppermute(value, "dp", [(0, 1), (1, 0)])


def partner_kind(me, other):
    step = jnp.abs(other - me)
    near = jnp.where(other == me ^ 1, SIDE, CROSS)
    distant = jnp.where(other == me ^ 2, FLIP, FAR)
    return jnp.where(step == 0, HERE, jnp.where(step == 1, near, distant))


def in_hbm(*values):
    return tuple(pltpu.with_memory_space_constraint(value, pltpu.HBM) for value in values)


def in_vmem(*values):
    return tuple(pltpu.with_memory_space_constraint(value, pltpu.VMEM) for value in values)


def in_smem(*values):
    return tuple(pltpu.with_memory_space_constraint(value, pltpu.SMEM) for value in values)


def tables_kernel(at_ref, starts_ref, owners_ref, owned_kind, owned_slot, held_kind, core):
    me = at_ref[0]
    core[0] = at_ref[1]
    devices, total = starts_ref.shape[0], owners_ref.shape[0]

    def tally(b, sums):
        owner = owners_ref[b]
        return sums[0] + (owner < me).astype(jnp.int32), sums[1] + (owner == me).astype(jnp.int32)

    zero = jnp.int32(0)
    first, count = lax.fori_loop(0, total, tally, (zero, zero))
    near = [me + step for step in range(-REACH, REACH + 1)]
    begins = [starts_ref[jnp.clip(device, 0, devices - 1)] for device in near]
    for j in range(owned_kind.shape[0]):
        holder, start = near[0], begins[0]
        for device, begin in zip(near, begins):
            reached = (device >= 0) & (device < devices) & (begin <= first + j)
            holder = jnp.where(reached, device, holder)
            start = jnp.where(reached, begin, start)
        owned_kind[j] = jnp.where(j < count, partner_kind(me, holder), -1)
        owned_slot[j] = jnp.clip(first + j - start, 0, held_kind.shape[0] - 1)
    start = starts_ref[me]
    end = jnp.where(me + 1 < devices, starts_ref[jnp.minimum(me + 1, devices - 1)], total)
    for s in range(held_kind.shape[0]):
        owner = owners_ref[jnp.minimum(start + s, total - 1)]
        held_kind[s] = jnp.where(start + s < end, partner_kind(me, owner), -1)


def tables(shard_starts, block_owners, at, slot_count, owned_slots):
    owned = pltpu.SMEM((owned_slots,), jnp.int32)
    return pl.pallas_call(
        tables_kernel,
        in_specs=[pl.BlockSpec(memory_space=pltpu.SMEM)] * 3,
        out_specs=[pl.BlockSpec(memory_space=pltpu.SMEM)] * 4,
        out_shape=[owned, owned]
        + [pltpu.SMEM((size,), jnp.int32) for size in (slot_count, 1)],
        compiler_params=pltpu.CompilerParams(vmem_limit_bytes=SMALL_VMEM),
        name="tables",
    )(at, *in_hbm(shard_starts, block_owners))


def split(value):
    high = value.astype(jnp.bfloat16)
    return high, (value - high.astype(jnp.float32)).astype(jnp.bfloat16)


def product(a, b, dims):
    return lax.dot_general(a, b, (dims, ((), ())), preferred_element_type=jnp.float32)


def product3(a, b, dims):
    count = a[0].shape[0]
    tall = product(jnp.concatenate(a, axis=0), b[0], dims)
    return tall[:count] + (tall[count:] + product(a[0], b[1], dims))


NN = ((1,), (0,))
NT = ((1,), (1,))


def prepare_kernel(place_ref, moment_ref, second_ref, left_ref, right_ref, *outs):
    turned_out, second_out, flip_high, flip_low, right_high, right_low, row_high, row_low = outs
    every = range(moment_ref.shape[0])
    half = row_high.shape[1]
    here = pl.multiple_of(place_ref[0] * half, half)
    right = [split(right_ref[g]) for g in every]
    first = [product3(split(moment_ref[g]), right[g], NN) for g in every]
    flipped = [split(left_ref[g].T) for g in every]
    turned = [product3(flipped[g], split(first[g]), NN) for g in every]
    for g in every:
        turned_out[g] = turned[g] * (beta_one / bias_one)
        second_out[g] = second_ref[g] * beta_two
        flip_high[g], flip_low[g] = flipped[g]
        right_high[g], right_low[g] = right[g]
        row_high[g], row_low[g] = split(left_ref[g, pl.ds(here, half)])


def prepare(place, first_moment, second_moment, left_basis, right_basis, half):
    count, width, _ = first_moment.shape
    group = PREPARE_GROUP if count % PREPARE_GROUP == 0 else 1
    spec = pl.BlockSpec((group, width, width), lambda j: (j, 0, 0))
    part = pl.BlockSpec((group, half, width), lambda j: (j, 0, 0))
    full = pltpu.VMEM(first_moment.shape, jnp.float32)
    short = pltpu.VMEM(first_moment.shape, jnp.bfloat16)
    rows = pltpu.VMEM((count, half, width), jnp.bfloat16)
    return pl.pallas_call(
        prepare_kernel,
        grid=(count // group,),
        in_specs=[pl.BlockSpec(memory_space=pltpu.SMEM)] + [spec] * 4,
        out_specs=[spec] * 6 + [part] * 2,
        out_shape=[full] * 2 + [short] * 4 + [rows] * 2,
        compiler_params=pltpu.CompilerParams(vmem_limit_bytes=STEP_VMEM),
        cost_estimate=pl.CostEstimate(
            flops=12 * count * width**3, bytes_accessed=16 * count * width**2, transcendentals=0
        ),
        name="prepare",
    )(place, *in_hbm(first_moment, second_moment, left_basis, right_basis))


def load_kernel(place_ref, source_ref, out_ref):
    out_ref[...] = source_ref[...]


def load_rows(place, source, half):
    count, _, width = source.shape
    return pl.pallas_call(
        load_kernel,
        grid_spec=pltpu.PrefetchScalarGridSpec(
            num_scalar_prefetch=1,
            grid=(1,),
            in_specs=[pl.BlockSpec((count, half, width), lambda _, place: (0, place[0], 0))],
            out_specs=pl.BlockSpec((count, half, width), lambda _, place: (0, 0, 0)),
        ),
        out_shape=pltpu.VMEM((count, half, width), source.dtype),
        compiler_params=pltpu.CompilerParams(vmem_limit_bytes=SMALL_VMEM),
        name="load_rows",
    )(place, *in_hbm(source))


def add_kernel(place_ref, mine_ref, other_ref, out_ref):
    half = out_ref.shape[1]
    rows = pl.ds(pl.multiple_of(place_ref[0] * half, half), half)
    for s in range(out_ref.shape[0]):
        total = mine_ref[s].astype(jnp.float32) + other_ref[s, rows].astype(jnp.float32)
        out_ref[s] = total.astype(out_ref.dtype)


def add_replicas(place, mine, other):
    return pl.pallas_call(
        add_kernel,
        in_specs=[pl.BlockSpec(memory_space=pltpu.SMEM)]
        + [pl.BlockSpec(memory_space=pltpu.VMEM)] * 2,
        out_specs=pl.BlockSpec(memory_space=pltpu.VMEM),
        out_shape=pltpu.VMEM(mine.shape, mine.dtype),
        compiler_params=pltpu.CompilerParams(vmem_limit_bytes=SMALL_VMEM),
        name="add_replicas",
    )(place, *in_vmem(mine, other))


def collect_kernel(kind_ref, slot_ref, *refs, kinds):
    sources, out_ref = refs[: len(kinds)], refs[-1]
    for j in range(out_ref.shape[0]):
        for kind, source in zip(kinds, sources):

            @pl.when(kind_ref[j] == kind)
            def _():
                out_ref[j] = source[slot_ref[j]]


def collect(kind, slot, sources, base):
    count = kind.shape[0]
    first = next(iter(sources.values()))
    extra = () if base is None else (base,)
    return pl.pallas_call(
        functools.partial(collect_kernel, kinds=tuple(sources)),
        in_specs=[pl.BlockSpec(memory_space=pltpu.SMEM)] * 2
        + [pl.BlockSpec(memory_space=pltpu.VMEM)] * (len(sources) + len(extra)),
        out_specs=pl.BlockSpec(memory_space=pltpu.VMEM),
        out_shape=pltpu.VMEM((count,) + first.shape[1:], first.dtype),
        input_output_aliases={2 + len(sources): 0} if extra else {},
        compiler_params=pltpu.CompilerParams(vmem_limit_bytes=SMALL_VMEM),
    )(*in_smem(kind, slot), *in_vmem(*sources.values(), *extra))


def rotate_kernel(mine_ref, right_high, right_low, high_ref, low_ref):
    for g in range(mine_ref.shape[0]):
        gradient = mine_ref[g]
        turned = product(gradient, right_high[g], NN) + product(gradient, right_low[g], NN)
        high_ref[g], low_ref[g] = split(turned)


def rotate_rows(mine, prepared):
    right = prepared[4:6]
    return pl.pallas_call(
        rotate_kernel,
        in_specs=[pl.BlockSpec(memory_space=pltpu.VMEM)] * 3,
        out_specs=[pl.BlockSpec(memory_space=pltpu.VMEM)] * 2,
        out_shape=[pltpu.VMEM(mine.shape, jnp.bfloat16)] * 2,
        compiler_params=pltpu.CompilerParams(vmem_limit_bytes=SMALL_VMEM),
        cost_estimate=pl.CostEstimate(
            flops=4 * mine.size * mine.shape[2], bytes_accessed=6 * mine.size, transcendentals=0
        ),
        name="rotate_rows",
    )(*in_vmem(mine, *right))


def step_kernel(kind_ref, slot_ref, place_ref, mine_high, mine_low, other_ref, *refs):
    turned_ref, second_ref, flip_high, flip_low, right_high, right_low, row_high, row_low = refs[:8]
    second_out, sends, codes, first_high, first_low = refs[8], refs[9:14], *refs[14:]
    step = pl.program_id(0)
    group, half = other_ref.shape[:2]
    here = pl.multiple_of(place_ref[0] * half, half)
    there = pl.multiple_of((1 - place_ref[0]) * half, half)
    every = range(group)

    @pl.when(step == 0)
    def _():
        codes[...] = jnp.zeros_like(codes)

    spots = lax.broadcasted_iota(jnp.int32, codes.shape[1:], 0)
    at = [dict() for _ in every]

    def rotate_right(g):
        gradient = other_ref[g]
        turned = product(gradient, right_high[g], NN) + product(gradient, right_low[g], NN)
        high, low = split(turned)
        first_high[g, pl.ds(here, half)], first_low[g, pl.ds(here, half)] = mine_high[g], mine_low[g]
        first_high[g, pl.ds(there, half)], first_low[g, pl.ds(there, half)] = high, low

    def rotate_left(g):
        first = (first_high[g], first_low[g])
        at[g]["turned"] = product3((flip_high[g], flip_low[g]), first, NN)

    def scale(g):
        turned = at[g].pop("turned")
        second = second_ref[g] + (1.0 - beta_two) * turned * turned
        second_out[g] = second
        unbiased = second * (1.0 / bias_two)
        root = unbiased * lax.rsqrt(unbiased)
        moment = turned_ref[g] + ((1.0 - beta_one) / bias_one) * turned
        at[g]["scaled"] = split(moment / (root + epsilon))

    def return_left(g):
        at[g]["back"] = product3((row_high[g], row_low[g]), at[g].pop("scaled"), NN)

    def return_right(g):
        at[g]["update"] = product3(split(at[g].pop("back")), (right_high[g], right_low[g]), NT)

    def quantize(g):
        update = at[g].pop("update")
        peak = jnp.max(jnp.abs(update), axis=0, keepdims=True)
        code = jnp.ceil(jnp.log2(jnp.maximum(peak, 1e-30) * (1.0 / 32000.0)) * CODE_STEPS)
        coded = jnp.round(update * jnp.exp2(code * (-1.0 / CODE_STEPS)))
        at[g]["coded"] = jnp.clip(coded, -32767.0, 32767.0).astype(jnp.int32).astype(jnp.int16)
        at[g]["code"] = code.astype(jnp.int32)

    def deliver(g):
        coded, code = at[g].pop("coded"), at[g].pop("code")
        slot = slot_ref[step * group + g]
        rows = pl.ds(pl.multiple_of(slot * half, half), half)
        for kind in range(5):

            @pl.when(kind_ref[step * group + g] == kind)
            def _():
                sends[kind][rows] = coded
                codes[kind] = jnp.where(spots == slot, code, codes[kind])

    stages = (rotate_right, rotate_left, scale, return_left, return_right, quantize)
    for wave in range(group + len(stages) - 1):
        for depth in reversed(range(len(stages))):
            if 0 <= wave - depth < group:
                stages[depth](wave - depth)
    for g in every:
        deliver(g)

    @pl.when(step == pl.num_programs(0) - 1)
    def _():
        for kind in range(5):
            top = sends[kind].shape[0] - CODE_ROWS
            sends[kind][pl.ds(top, CODE_ROWS)] = codes[kind].astype(jnp.int16)


def soap_step(kind, slot, place, rotated, other, prepared, slot_count):
    count, half, width = other.shape
    group = GROUP if count % GROUP == 0 else 1
    full = pl.BlockSpec((group, width, width), lambda j: (j, 0, 0))
    part = pl.BlockSpec((group, half, width), lambda j: (j, 0, 0))
    send_rows = slot_count * half + CODE_ROWS
    send = pl.BlockSpec((send_rows, width), lambda j: (0, 0))
    return pl.pallas_call(
        step_kernel,
        grid=(count // group,),
        in_specs=[pl.BlockSpec(memory_space=pltpu.SMEM)] * 3
        + [part] * 3
        + [full] * 6
        + [part] * 2,
        out_specs=[full] + [send] * 5,
        scratch_shapes=[
            pltpu.VMEM((5, CODE_ROWS, width), jnp.int32),
            pltpu.VMEM((group, width, width), jnp.bfloat16),
            pltpu.VMEM((group, width, width), jnp.bfloat16),
        ],
        out_shape=[pltpu.VMEM((count, width, width), jnp.float32)]
        + [pltpu.VMEM((send_rows, width), jnp.int16)] * 5,
        compiler_params=pltpu.CompilerParams(vmem_limit_bytes=STEP_VMEM),
        name="soap_step",
    )(*in_smem(kind, slot, place), *in_vmem(*rotated, other, *prepared))


def finish_kernel(kind_ref, place_ref, mine_ref, other_ref, moment_ref, second_ref, *outs):
    first_out, second_out = outs
    j = pl.program_id(0)
    half = mine_ref.shape[1]
    live = kind_ref[j] >= 0
    for place, part in ((place_ref[0], mine_ref), (1 - place_ref[0], other_ref)):
        rows = pl.ds(pl.multiple_of(place * half, half), half)
        gradient = part[0].astype(jnp.float32)
        moment = beta_one * moment_ref[0, rows] + (1.0 - beta_one) * gradient
        first_out[0, rows] = jnp.where(live, moment, 0.0)
    second_out[0] = jnp.where(live, second_ref[0], 0.0)


def finish(kind, place, mine, other, first_moment, second):
    count, width, _ = first_moment.shape
    half = mine.shape[1]
    full = pl.BlockSpec((1, width, width), lambda j: (j, 0, 0))
    part = pl.BlockSpec((1, half, width), lambda j: (j, 0, 0))
    return pl.pallas_call(
        finish_kernel,
        grid=(count,),
        in_specs=[pl.BlockSpec(memory_space=pltpu.SMEM)] * 2 + [part, part, full, full],
        out_specs=[full] * 2,
        out_shape=[pltpu.HBM(first_moment.shape, jnp.float32)] * 2,
        compiler_params=pltpu.CompilerParams(vmem_limit_bytes=SMALL_VMEM),
        cost_estimate=pl.CostEstimate(
            flops=12 * count * width**2, bytes_accessed=12 * count * width**2, transcendentals=0
        ),
        name="finish",
    )(*in_smem(kind, place), *in_vmem(mine, other), *in_hbm(first_moment), *in_vmem(second))


def gather_kernel(kind_ref, *refs):
    sources, out_ref = refs[:5], refs[5]
    count = kind_ref.shape[0]
    top = out_ref.shape[0] - CODE_ROWS
    half = top // count
    spots = lax.broadcasted_iota(jnp.int32, (CODE_ROWS, out_ref.shape[1]), 0)
    chosen = jnp.zeros(spots.shape, jnp.int32)
    for s in range(count):
        for kind in range(5):

            @pl.when(kind_ref[s] == kind)
            def _():
                rows = pl.ds(s * half, half)
                out_ref[rows] = sources[kind][rows]

    for kind in range(5):
        code = sources[kind][pl.ds(top, CODE_ROWS)].astype(jnp.int32)
        for s in range(count):
            chosen = jnp.where((spots == s) & (kind_ref[s] == kind), code, chosen)
    out_ref[pl.ds(top, CODE_ROWS)] = chosen.astype(jnp.int16)


def gather_held(kind, sources):
    return pl.pallas_call(
        gather_kernel,
        in_specs=[pl.BlockSpec(memory_space=pltpu.SMEM)]
        + [pl.BlockSpec(memory_space=pltpu.VMEM)] * 5,
        out_specs=pl.BlockSpec(memory_space=pltpu.VMEM),
        out_shape=jax.ShapeDtypeStruct(sources[0].shape, sources[0].dtype),
        compiler_params=pltpu.CompilerParams(vmem_limit_bytes=SMALL_VMEM),
        name="gather_held",
    )(*in_smem(kind), *sources)


def decode_kernel(kind_ref, core_ref, coded_ref, *refs, twin):
    out_ref, values, sems = refs[-3:]
    count, half = values.shape[:2]
    top = count * half
    place = 1 - core_ref[0] if twin else core_ref[0]
    to = pl.ds(pl.multiple_of(place * half, half), half)
    code = coded_ref[pl.ds(top, CODE_ROWS)].astype(jnp.int32).astype(jnp.float32)
    scales = jnp.exp2(code * (1.0 / CODE_STEPS))
    copies = []
    for s in range(count):
        value = coded_ref[pl.ds(s * half, half)].astype(jnp.int32).astype(jnp.float32)
        values[s] = jnp.where(kind_ref[s] >= 0, value * scales[s : s + 1], 0.0)
        copies.append(pltpu.make_async_copy(values.at[s], out_ref.at[s, to], sems.at[s]))
        copies[-1].start()
    for copy in copies:
        copy.wait()


def decode(kind, core, coded, base, width):
    count = kind.shape[0]
    half = (coded.shape[0] - CODE_ROWS) // count
    twin = base is not None
    return pl.pallas_call(
        functools.partial(decode_kernel, twin=twin),
        in_specs=[pl.BlockSpec(memory_space=pltpu.SMEM)] * 2
        + [pl.BlockSpec(memory_space=pltpu.VMEM)]
        + [pl.BlockSpec(memory_space=pltpu.HBM)] * twin,
        out_specs=pl.BlockSpec(memory_space=pltpu.HBM),
        out_shape=pltpu.HBM((count, width, width), jnp.float32),
        input_output_aliases={3: 0} if twin else {},
        scratch_shapes=[
            pltpu.VMEM((count, half, width), jnp.float32),
            pltpu.SemaphoreType.DMA((count,)),
        ],
        compiler_params=pltpu.CompilerParams(vmem_limit_bytes=SMALL_VMEM),
        cost_estimate=pl.CostEstimate(
            flops=count * half * width, bytes_accessed=6 * count * half * width, transcendentals=0
        ),
        name="decode_twin" if twin else "decode_own",
    )(*in_smem(kind, core), coded, *((base,) if twin else ()))


def body(
    gradients, first_moment, second_moment, left_basis, right_basis, shard_starts, block_owners
):
    me = lax.axis_index("fsdp").astype(jnp.int32)
    core = lax.axis_index("dp").astype(jnp.int32)
    devices = lax.axis_size("fsdp")
    slot_count, width = gradients.shape[1], gradients.shape[3]
    owned_slots = first_moment.shape[0]
    half = width // lax.axis_size("dp")
    side, cross, flip, far = partner_pairs(devices)
    place = core.reshape(1)

    own_kind, own_slot, held_kind, core_index = tables(
        shard_starts, block_owners, jnp.stack((me, core)), slot_count, owned_slots
    )
    replica = gradients[0]
    twin = swap_cores(replica)

    summed = add_replicas(place, load_rows(place, replica, half), twin)
    by_flip = exchange(summed, flip)
    by_cross = exchange(summed, cross)
    by_far = exchange(summed, far)
    by_side = exchange(summed, side)
    prepared = prepare(place, first_moment, second_moment, left_basis, right_basis, half)
    sooner = {HERE: summed, SIDE: by_side, CROSS: by_cross, FAR: by_far}
    mine = collect(own_kind, own_slot, sooner, None)
    mine = collect(own_kind, own_slot, {FLIP: by_flip}, mine)
    other = swap_cores(mine)
    second, keep, to_side, to_cross, to_flip, to_far = soap_step(
        own_kind, own_slot, core_index, rotate_rows(mine, prepared), other, prepared, slot_count
    )
    first_new, second_new = finish(own_kind, core_index, mine, other, first_moment, second)
    sent = (
        keep,
        exchange(to_side, side),
        exchange(to_cross, cross),
        exchange(to_flip, flip),
        exchange(to_far, far),
    )
    coded = gather_held(held_kind, sent)
    twin_coded = swap_cores(coded)
    direction = decode(held_kind, core_index, coded, None, width)
    direction = decode(held_kind, core_index, twin_coded, direction, width)
    return (direction, first_new, second_new)


def solution(mesh):
    in_specs = (
        P("dp", "fsdp", None, None),
        P("fsdp", None, None),
        P("fsdp", None, None),
        P("fsdp", None, None),
        P("fsdp", None, None),
        P(),
        P(),
    )
    out_specs = (P("fsdp", None, None), P("fsdp", None, None), P("fsdp", None, None))
    return jax.shard_map(body, mesh=mesh, in_specs=in_specs, out_specs=out_specs, check_vma=False)
```
